32 devices in a mesh: space: 16 (over z, y, x), level: 2 (over core).
Axes of the slice: x: 2, y: 2, z: 4, core: 2. Of those that a mesh axis runs over, the one named last changes fastest.
Arguments:
- velocity: float32 [2, 16, 16384], P(None, 'level', 'space'), may hold values from -3 to 3
- density: float32 [16, 16384], P('level', 'space'), may hold values from -6 to 6
- elevation: float32 [16384], P('space'), may hold values from -3 to 3
- grad_weights: float32 [2, 6, 16384], P(None, None, 'space'), may hold values from -2.4 to 2.4
- lap_weights: float32 [6, 16384], P(None, 'space'), may hold values from 0.02 to 0.2
- coriolis: float32 [16384], P('space'), may hold values from 0.5 to 2
- node_area: float32 [16384], P('space'), may hold values from 1 to 100, as said below
- thickness: float32 [16], P('level'), may hold values from 0.5 to 2
- send_list: int32 [16, 256], P('space'), may hold values from 0 to 1023
- neighbours: int32 [6, 16384], P(None, 'space'), may hold values from 0 to 1279
- bottom: int32 [16384], P('space'), may hold values from 0 to 16, as said below
Outputs:
- velocity_out: float32 [2, 16, 16384], P(None, 'level', 'space')
- density_out: float32 [16, 16384], P('level', 'space')
- elevation_out: float32 [16384], P('space')
- volume_drift: float32 [4], replicated
The draws below stay inside these ranges and needn't reach their ends.
Inputs may be any that keep to these rules, and one draw needn't show every extreme that they name: `send_list`: local node numbers within the sending partition; the first 128 go to the partition one below along space, the other 128 to the one above. `neighbours`: slots below 1024 are the partition's own nodes; the next 128 are halo slots filled from the partition below, the last 128 from the partition above. Levels of a node are wet from the surface down to bottom - 1; a node with 0 is dry. Some partitions are shallower than others. `node_area`: positive areas.
All inputs are finite; a program needn't handle non-finite values.
Results may differ from the reference program's by a relative error of at most 0.00013.
Values sent between devices are 32-bit elements; how exact they have to be, the bound alone decides.
A program may use at most 64 MiB of HBM per device.

```python
import math
import jax
import jax.numpy as jnp
from jax import lax

NODES_DEV = 1024
HALO = 128
K = 6
STEPS = 4
NODES = 16384
LEVELS = 16
N_SPACE = 16


def draw_bottom(key, part):
    key_part = jax.random.fold_in(key, 11)
    key_node = jax.random.fold_in(key, 12)
    partitions = NODES // NODES_DEV
    shallow = jax.random.randint(key_part, (partitions, 1), LEVELS // 4, LEVELS + 1)
    shallow = shallow.at[0].set(LEVELS)
    depths = jax.random.randint(key_node, (partitions, NODES_DEV), 0, LEVELS + 1)
    return jnp.minimum(depths, shallow).reshape(NODES).astype(jnp.int32)


def draw_node_area(key, part):
    key_rough = jax.random.fold_in(key, 21)
    partitions = NODES // NODES_DEV
    owner = (jnp.arange(NODES, dtype=jnp.int32) // NODES_DEV).astype(jnp.float32)
    position = owner / jnp.float32(max(partitions - 1, 1))
    ramp = jnp.exp(jnp.log(jnp.float32(10.0)) * position)
    rough = jnp.exp(jax.random.uniform(key_rough, (NODES,), jnp.float32, 0.0, jnp.log(3.0)))
    return (ramp * rough).astype(jnp.float32)


def plant(values, rng, smallest, high):
    spot = [jax.random.randint(jax.random.fold_in(rng, axis), (), 0, length) for axis, length in enumerate(values.shape)]
    longest = values.shape.index(max(values.shape))
    neighbour = spot[:longest] + [(spot[longest] + 1) % values.shape[longest]] + spot[longest + 1:]
    return values.at[tuple(spot)].set(smallest).at[tuple(neighbour)].set(high)


def block_levels(rng, extent, pieces, smallest, top_value):
    loudness, own = 1.0, jax.random.fold_in(rng, 6)
    for dim, blocks in pieces:
        heights = jnp.exp(jax.random.uniform(jax.random.fold_in(own, dim), (blocks,), jnp.float32, smallest / len(pieces), top_value / len(pieces)))
        loudness = loudness * jnp.repeat(heights, extent[dim] // blocks).reshape([-1 if axis == dim else 1 for axis in range(len(extent))])
    return loudness


def scatter_about(rng, shape, width, most, shards=(), held_as=jnp.bfloat16):
    loudness = block_levels(rng, shape, shards, -0.22, 0.18) if shards else 1.0
    values = jax.random.normal(rng, shape, jnp.float32) * width * loudness
    return jnp.minimum(jnp.maximum(values, -most), most).astype(held_as)


def setup_inputs(seed: int = 0) -> dict:
    key_list = jax.random.split(jax.random.key(seed), 12)
    return {
        "velocity": scatter_about(key_list[0], (2, LEVELS, NODES), 0.5, 3.0, ((1, 2), (2, 16)), jnp.float32),
        "density": scatter_about(key_list[1], (LEVELS, NODES), 1.0, 6.0, ((0, 2), (1, 16)), jnp.float32),
        "elevation": scatter_about(key_list[2], (NODES,), 0.5, 3.0, ((0, 16),), jnp.float32),
        "grad_weights": scatter_about(key_list[3], (2, K, NODES), 0.4, 2.4, ((2, 16),), jnp.float32),
        "lap_weights": jnp.clip(jnp.exp(math.log(0.2) - 2.3025851 * jax.random.uniform(key_list[4], (K, NODES), jnp.float32) ** block_levels(key_list[4], (K, NODES), ((1, 16),), -0.2, 0.2)), 0.02, 0.2),
        "coriolis": jnp.clip(jnp.exp(math.log(2.0) - 1.3862944 * jax.random.uniform(key_list[5], (NODES,), jnp.float32) ** block_levels(key_list[5], (NODES,), ((0, 16),), -0.2, 0.2)), 0.5, 2.0),
        "node_area": draw_node_area(jax.random.fold_in(key_list[11], 71), 0),
        "thickness": jnp.clip(jnp.exp(math.log(2.0) - 1.3862944 * jax.random.uniform(key_list[7], (LEVELS,), jnp.float32) ** block_levels(key_list[7], (LEVELS,), ((0, 2),), -0.2, 0.2)), 0.5, 2.0),
        "send_list": plant(jax.random.randint(key_list[8], (N_SPACE, 2 * HALO), 0, NODES_DEV), jax.random.fold_in(key_list[8], 1), 0, NODES_DEV - 1).astype(jnp.int32),
        "neighbours": plant(jax.random.randint(key_list[9], (K, NODES), 0, NODES_DEV + 2 * HALO), jax.random.fold_in(key_list[9], 1), 0, (NODES_DEV + 2 * HALO) - 1).astype(jnp.int32),
        "bottom": draw_bottom(jax.random.fold_in(key_list[11], 71), 0),
    }


time_step = 0.1
buoyancy = 0.5
drag_rate = 0.5


def neighbour_table(send_list, neighbours):
    node_ids = jnp.arange(NODES, dtype=jnp.int32)
    owner = (node_ids // NODES_DEV)[None, :]
    slot_index = neighbours
    source_below = jnp.clip(owner - 1, 0, N_SPACE - 1)
    source_above = jnp.clip(owner + 1, 0, N_SPACE - 1)
    local_below = send_list[source_below, jnp.clip(HALO + slot_index - NODES_DEV, 0, 2 * HALO - 1)]
    local_above = send_list[source_above, jnp.clip(slot_index - NODES_DEV - HALO, 0, 2 * HALO - 1)]
    global_index = jnp.where(slot_index < NODES_DEV, owner * NODES_DEV + slot_index,
                             jnp.where(slot_index < NODES_DEV + HALO, source_below * NODES_DEV + local_below,
                                       source_above * NODES_DEV + local_above))
    is_valid = jnp.where(slot_index < NODES_DEV, True,
                         jnp.where(slot_index < NODES_DEV + HALO, owner >= 1, owner <= N_SPACE - 2))
    return global_index.astype(jnp.int32), is_valid.astype(jnp.float32)


def stencil(fields, global_index, weight):
    result = jnp.zeros_like(fields)
    for column in range(K):
        nearby = jnp.take(fields, global_index[column], axis=-1)
        result = result + weight[column] * (nearby - fields)
    return result


def reference(velocity, density, elevation, grad_weights, lap_weights, coriolis, node_area, thickness, send_list, neighbours, bottom):
    global_index, valid_float = neighbour_table(send_list, neighbours)
    east_weight = grad_weights[0] * valid_float
    north_weight = grad_weights[1] * valid_float
    smooth_weight = lap_weights * valid_float
    level_ids = jnp.arange(LEVELS, dtype=jnp.int32)[:, None]
    wet_cells = (level_ids < bottom[None, :]).astype(jnp.float32)
    at_floor = (level_ids == bottom[None, :] - 1).astype(jnp.float32)
    wet_nodes = (bottom > 0).astype(jnp.float32)
    area_total = jnp.sum(node_area * wet_nodes)
    velocity = velocity * wet_cells[None]
    drifts = []
    for counter in range(STEPS):
        east_speed = velocity[0]
        north_speed = velocity[1]
        weighted = density * thickness[:, None]
        pressure = buoyancy * (jnp.cumsum(weighted, axis=0) - 0.5 * weighted)
        transport = jnp.einsum('cln,l->cn', velocity, thickness, precision=lax.Precision.HIGHEST)
        diverge = stencil(transport[0], global_index, east_weight) + stencil(transport[1], global_index, north_weight)
        drift = jnp.sum(node_area * wet_nodes * diverge) / area_total
        drifts.append(drift)
        new_elevation = elevation - time_step * wet_nodes * diverge + time_step * drift
        slope_east = stencil(elevation, global_index, east_weight)
        slope_north = stencil(elevation, global_index, north_weight)
        press_east = stencil(pressure, global_index, east_weight)
        press_north = stencil(pressure, global_index, north_weight)
        smooth_speed = stencil(velocity.reshape(2 * LEVELS, NODES), global_index, smooth_weight)
        push_east = (-slope_east[None] - press_east + coriolis[None] * north_speed
                     + smooth_speed[:LEVELS] - drag_rate * at_floor * east_speed)
        push_north = (-slope_north[None] - press_north - coriolis[None] * east_speed
                      + smooth_speed[LEVELS:] - drag_rate * at_floor * north_speed)
        dense_east = stencil(density, global_index, east_weight)
        dense_north = stencil(density, global_index, north_weight)
        dense_smooth = stencil(density, global_index, smooth_weight)
        density = density + time_step * (dense_smooth - east_speed * dense_east - north_speed * dense_north)
        velocity = wet_cells[None] * (velocity + time_step * jnp.stack([push_east, push_north]))
        elevation = new_elevation
    return velocity, density, elevation, jnp.stack(drifts).astype(jnp.float32)
```

```python
import functools

import jax
import jax.numpy as jnp
from jax import lax
from jax.experimental import pallas as pl
from jax.experimental.pallas import tpu as pltpu
from jax.sharding import PartitionSpec as P

STEPS = 4
LANES = 128

time_step = 0.1
buoyancy = 0.5
drag_rate = 0.5


def lane_gather(values, lanes):
    return jnp.take_along_axis(values, lanes, axis=1, mode="promise_in_bounds")


def pick(tiles, lanes, masks):
    found = lane_gather(tiles[0], lanes)
    for tile, mask in zip(tiles[1:], masks):
        found = jnp.where(mask, lane_gather(tile, lanes), found)
    return found


def running_sum(values, rows, row_ids):
    shift = 1
    while shift < rows:
        moved = pltpu.roll(values, shift, 0)
        values = values + jnp.where(row_ids >= shift, moved, 0.0)
        shift *= 2
    return values


def spread_sum(values):
    shift = values.shape[0] // 2
    while shift:
        values = values + pltpu.roll(values, shift, 0)
        shift //= 2
    return values


def kernel(
    n_space, n_level, width, rows, blocks, near_count,
    vel, den, ele, grad, lap, cor, area, thick, send, near, bot,
    vel_out, den_out, ele_out, drift_out,
    own, eta, lanes_of, block_of, weight_of, q_lanes, q_block, q_weight,
    part, q_part, q_of, q_sum, small, out, out_small, halo, halo_small, peer_out, peer,
    vol, vol_line, vol_all,
    main_send, main_recv, hs_send, hs_recv, peer_send, peer_recv, vol_send, vol_recv, column_in,
    load_sem, thick_in, *loaded,
):
    sp = lax.axis_index("space")
    lv = lax.axis_index("level")
    n_dev = n_space * n_level
    has = (sp > 0, sp < n_space - 1)
    ends = (sp - 1, sp + 1)
    low = jnp.where(has[0], 1, 0)
    high = jnp.where(has[1], 1, 0)
    others = [lax.rem(lv + d, n_level) for d in range(1, n_level)]

    barrier = pltpu.get_barrier_semaphore()

    mine, place = sp // width, lax.rem(sp, width)
    column = [(lax.rem(sp + d * width, n_space), lv) for d in range(1, n_space // width)]
    row = [(mine * width + lax.rem(place + d, width), lax.rem(lv + e, n_level))
           for d in range(width) for e in range(n_level) if d or e]
    for q, level in row + column:
        pl.semaphore_signal(barrier, inc=1, device_id={"space": q, "level": level})
    for side in range(2):
        @pl.when(has[side])
        def _():
            for q in [lv] + others:
                pl.semaphore_signal(barrier, inc=1, device_id={"space": ends[side], "level": q})

    loads = [
        pltpu.make_async_copy(ref, buffer, load_sem.at[i])
        for i, (ref, buffer) in enumerate(zip(
            (vel, den, ele, grad, lap, cor, area, thick, send, near, bot),
            loaded[:7] + (thick_in,) + loaded[7:]))
    ]
    for load in loads:
        load.start()

    row_ids = lax.broadcasted_iota(jnp.int32, (rows, LANES), 0)
    eight = lax.broadcasted_iota(jnp.int32, (8, LANES), 0)
    odd = jnp.bitwise_and(eight, 1) == 1
    lane_ids = lax.broadcasted_iota(jnp.int32, (1, LANES), 1)
    level_ids = row_ids + lv * rows

    def wide(row, count=rows):
        return jnp.broadcast_to(row, (count, LANES))

    for side in range(2):
        @pl.when(jnp.logical_not(has[side]))
        def _():
            halo[:, side] = jnp.zeros(halo.shape[:1] + halo.shape[2:], jnp.float32)
            halo_small[:, side] = jnp.zeros(halo_small.shape[:1] + halo_small.shape[2:], jnp.float32)

    for load in loads:
        load.wait()
    vel, den, ele, grad, lap, cor, area, send, near, bot = loaded

    thickness = jnp.zeros((rows, LANES), jnp.float32)
    for r in range(rows):
        thickness = jnp.where(row_ids == r, thick_in[r], thickness)

    def prepare(t, _):
        here = pl.ds(pl.multiple_of(t * LANES, LANES), LANES)
        wet = level_ids < wide(bot[pl.ds(t, 1), :])
        own[0, t] = jnp.where(wet, vel[0, :, here], 0.0)
        own[1, t] = jnp.where(wet, vel[1, :, here], 0.0)
        own[2, t] = den[:, here]
        eta[t] = jnp.where(lv == 0, wide(ele[pl.ds(t, 1), :], 8), 0.0)
        lane_pack = jnp.zeros((8, LANES), jnp.int32)
        block_pack = jnp.zeros((8, LANES), jnp.int32)
        packs = [jnp.zeros((8, LANES), jnp.float32) for _ in range(4)]
        for k in range(near_count):
            slot = wide(near[k:k + 1, here])
            block = lax.shift_right_logical(slot, 7)
            lanes = jnp.bitwise_and(slot, LANES - 1)
            inside = block < blocks
            outside = jnp.where(inside, 0, jnp.where(block == blocks, low, high)) > 0
            lanes_of[t, k] = lanes
            block_of[t, k] = block
            values = (wide(grad[k, 0:1, here]), wide(grad[k, 1:2, here]), wide(lap[k:k + 1, here]))
            picked = [jnp.where(mask, value, 0.0) for mask in (inside, outside) for value in values]
            for i in range(6):
                weight_of[t, k, i] = picked[i]
            mine = eight == k
            lane_pack = jnp.where(mine, lanes[:8], lane_pack)
            block_pack = jnp.where(mine, block[:8], block_pack)
            packs = [jnp.where(mine, picked[i][:8], pack) for i, pack in zip((0, 1, 3, 4), packs)]
        q_lanes[t] = lane_pack
        q_block[t] = block_pack
        for i in range(4):
            q_weight[t, i] = packs[i]
        return 0

    lax.fori_loop(0, blocks, prepare, 0)
    wet_area = area[...] * jnp.where(bot[...] > 0, 1.0, 0.0)
    count = jnp.where(lv == 0, 1.0, 0.0)
    vol[...] = jnp.where(eight == STEPS, wide(jnp.sum(wet_area, axis=0, keepdims=True), 8) * count, 0.0)

    def version(q):
        return jnp.where(q > lv, 1, 0)

    def main_copy(s, side):
        return pltpu.make_async_remote_copy(
            src_ref=out.at[s, side], dst_ref=halo.at[s, 1 - side],
            send_sem=main_send.at[s, side], recv_sem=main_recv.at[s, 1 - side],
            device_id={"space": ends[side], "level": lv}, device_id_type=pl.DeviceIdType.MESH)

    def small_copy(s, side, q, slot):
        return pltpu.make_async_remote_copy(
            src_ref=out_small.at[s, side, version(q)], dst_ref=halo_small.at[s, 1 - side, slot],
            send_sem=hs_send.at[s, side, q], recv_sem=hs_recv.at[s, 1 - side, slot],
            device_id={"space": ends[side], "level": q}, device_id_type=pl.DeviceIdType.MESH)

    def peer_copy(s, q, slot):
        return pltpu.make_async_remote_copy(
            src_ref=peer_out.at[s, jnp.where(s < STEPS, version(q), 0)], dst_ref=peer.at[s, slot],
            send_sem=peer_send.at[s, q], recv_sem=peer_recv.at[s, slot],
            device_id={"space": sp, "level": q}, device_id_type=pl.DeviceIdType.MESH)

    dev = sp * n_level + lv

    def vol_copy(q, slot):
        return pltpu.make_async_remote_copy(
            src_ref=vol_line, dst_ref=vol_all.at[slot],
            send_sem=vol_send.at[q], recv_sem=vol_recv.at[slot],
            device_id={"space": q // n_level, "level": lax.rem(q, n_level)},
            device_id_type=pl.DeviceIdType.MESH)

    def scalars(t, rho, level):
        heavy = level + buoyancy * spread_sum(rho * thickness)
        small[t] = jnp.where(odd, heavy, level)
        return heavy

    def stage_out(s):
        for side in range(2):
            slot = wide(send[:, side * LANES:(side + 1) * LANES])
            lanes = jnp.bitwise_and(slot, LANES - 1)
            block = lax.shift_right_logical(slot, 7)
            masks = [block == b for b in range(1, blocks)]
            for g in range(3):
                out[s, side, g * rows:(g + 1) * rows] = pick([own[g, b] for b in range(blocks)], lanes, masks)
            found = pick([small[b] for b in range(blocks)], lanes[:8], [m[:8] for m in masks])
            out[s, side, 3 * rows:3 * rows + 8] = found
            for i in range(2):
                out_small[s, side, i] = found[i:i + 1]

    def send_out(s):
        for side in range(2):
            @pl.when(has[side])
            def _():
                main_copy(s, side).start()
                for q in others:
                    small_copy(s, side, q, lv).start()
        for q in others:
            peer_copy(s, q, lv).start()

    def close(s):
        for q in others:
            peer_copy(s, q, lv).wait_send()
        for side in range(2):
            @pl.when(has[side])
            def _():
                main_copy(s, side).wait_send()
                for q in others:
                    small_copy(s, side, q, lv).wait_send()

    def own_parts():
        def body(t, _):
            tiles = [[own[g, b] for b in range(blocks)] for g in range(3)]
            here = [own[g, t] for g in range(3)]
            zero = jnp.zeros((rows, LANES), jnp.float32)
            sums = [zero] * 6
            for k in range(near_count):
                block = block_of[t, k]
                masks = [block == b for b in range(1, blocks)]
                diff = [pick(tiles[g], lanes_of[t, k], masks) - here[g] for g in range(3)]
                sums = gathered(sums, diff, [weight_of[t, k, i] for i in range(3)])
            for i in range(6):
                part[t, i] = sums[i]
            return 0
        lax.fori_loop(0, blocks, body, 0)

    def gathered(sums, diff, weights):
        east, north, smooth = weights
        return [sums[0] + smooth * diff[0], sums[1] + smooth * diff[1], sums[2] + smooth * diff[2],
                sums[3] + east * diff[2], sums[4] + north * diff[2],
                sums[5] + (east * diff[0] + north * diff[1])]

    def own_surface(s):
        total = peer_out[s, 0]
        for q in others:
            total = total + peer[s, q]
        q_sum[...] = total
        for t in range(blocks):
            q_of[t] = wide(q_sum[t:t + 1, :], 8)
        tiles = [q_of[b] for b in range(blocks)]
        for t in range(blocks):
            block = q_block[t]
            diff = pick(tiles, q_lanes[t], [block == b for b in range(1, blocks)]) - tiles[t]
            q_part[t, 0] = q_weight[t, 0] * diff
            q_part[t, 1] = q_weight[t, 1] * diff

    def receive(s):
        for side in range(2):
            @pl.when(has[side])
            def _():
                main_copy(s, 1 - side).wait_recv()
                for q in others:
                    small_copy(s, 1 - side, q, q).wait_recv()
        for side in range(2):
            total = halo[s, side, 3 * rows:3 * rows + 1]
            for q in others:
                total = total + halo_small[s, side, q]
            q_of[blocks + side] = wide(total, 8)

    def finish(s):
        edges = [[halo[s, side, g * rows:(g + 1) * rows] for side in range(2)] for g in range(3)]
        edges.append([q_of[blocks], q_of[blocks + 1]])

        def body(t, carry):
            volume, light, heavy = carry
            here = [own[g, t] for g in range(3)]
            sums = [part[t, i] for i in range(6)]
            for k in range(near_count):
                lanes = lanes_of[t, k]
                upper = block_of[t, k] == blocks + 1
                diff = [jnp.where(upper, lane_gather(edges[g][1], lanes), lane_gather(edges[g][0], lanes)) - here[g]
                        for g in range(3)]
                sums = gathered(sums, diff, [weight_of[t, k, 3 + i] for i in range(3)])
            lap0, lap1, lap2, east2, north2, flow = sums
            lanes = q_lanes[t]
            diff = jnp.where(q_block[t] == blocks + 1, lane_gather(edges[3][1], lanes),
                             lane_gather(edges[3][0], lanes)) - q_of[t]
            slope0 = spread_sum(q_part[t, 0] + q_weight[t, 2] * diff)
            slope1 = spread_sum(q_part[t, 1] + q_weight[t, 3] * diff)
            bottom = wide(bot[pl.ds(t, 1), :])
            turn = wide(cor[pl.ds(t, 1), :])
            drag = jnp.where(level_ids == bottom - 1, drag_rate, 0.0)
            u, v, rho = here
            east3, north3 = thickness * east2, thickness * north2
            east3 = slope0 + buoyancy * (running_sum(east3, rows, row_ids) - 0.5 * east3)
            north3 = slope1 + buoyancy * (running_sum(north3, rows, row_ids) - 0.5 * north3)
            push0 = -east3 + turn * v + lap0 - drag * u
            push1 = -north3 - turn * u + lap1 - drag * v
            wet = level_ids < bottom
            own[0, t] = jnp.where(wet, u + time_step * push0, 0.0)
            own[1, t] = jnp.where(wet, v + time_step * push1, 0.0)
            fresh = rho + time_step * (lap2 - u * east2 - v * north2)
            own[2, t] = fresh
            diverge = jnp.where(bottom[:8] > 0, spread_sum(thickness * flow), 0.0)
            level = eta[t] - time_step * diverge
            eta[t] = level
            dense = scalars(t, fresh, level)
            return (volume + wide(area[pl.ds(t, 1), :], 8) * diverge,
                    jnp.where(eight == t, level, light), jnp.where(eight == t, dense, heavy))

        zero = jnp.zeros((8, LANES), jnp.float32)
        volume, light, heavy = lax.fori_loop(0, blocks, body, (zero, zero, zero), unroll=True)
        vol[...] = jnp.where(eight == s, volume, vol[...])
        peer_out[s + 1, 0] = light
        peer_out[s + 1, 1] = heavy

    def first(t, carry):
        light, heavy = carry
        dense = scalars(t, own[2, t], eta[t])
        return jnp.where(eight == t, eta[t], light), jnp.where(eight == t, dense, heavy)

    zero = jnp.zeros((8, LANES), jnp.float32)
    light, heavy = lax.fori_loop(0, blocks, first, (zero, zero), unroll=True)
    peer_out[0, 0] = light
    peer_out[0, 1] = heavy
    stage_out(0)

    expected = len(row) + len(column) + n_level * (low + high)
    pl.semaphore_wait(barrier, expected)
    for q, level in row:
        pl.semaphore_signal(column_in, inc=1, device_id={"space": q, "level": level})

    def step(s, _):
        send_out(s)
        own_parts()
        for q in others:
            peer_copy(s, q, q).wait_recv()
        own_surface(s)
        receive(s)
        finish(s)

        @pl.when(s < STEPS - 1)
        def _():
            stage_out(s + 1)

        close(s)
        return 0

    lax.fori_loop(0, STEPS, step, 0)

    sums = jnp.sum(vol[...], axis=1, keepdims=True)
    line = jnp.zeros((1, LANES), jnp.float32)
    for i in range(STEPS + 1):
        line = jnp.where(lane_ids == i, sums[i:i + 1], line)
    vol_line[...] = line
    pl.semaphore_wait(column_in, len(row))
    for q in others:
        peer_copy(STEPS, q, lv).start()

    def start(d, _):
        vol_copy(lax.rem(dev + d, n_dev), dev).start()
        return 0

    lax.fori_loop(1, n_dev, start, 0)

    for t in range(blocks):
        here = slice(t * LANES, (t + 1) * LANES)
        vel_out[0, :, here] = own[0, t]
        vel_out[1, :, here] = own[1, t]
        den_out[:, here] = own[2, t]

    level = peer_out[STEPS, 0]
    for q in others:
        peer_copy(STEPS, q, q).wait_recv()
        level = level + peer[STEPS, q]

    def collect(d, total):
        q = lax.rem(dev + d, n_dev)
        vol_copy(q, q).wait_recv()
        return total + vol_all[q]

    total = lax.fori_loop(1, n_dev, collect, vol_line[...])
    drifts = total / total[:, STEPS:STEPS + 1]
    shift = jnp.sum(jnp.where(lane_ids < STEPS, drifts, 0.0), axis=1, keepdims=True)
    ele_out[...] = level + time_step * shift
    drift_out[...] = drifts
    for q in others:
        peer_copy(STEPS, q, lv).wait_send()

    def done(d, _):
        vol_copy(lax.rem(dev + d, n_dev), dev).wait_send()
        return 0

    lax.fori_loop(1, n_dev, done, 0)


def emit(vel, den, ele, drift, vel_out, den_out, ele_out, drift_out):
    vel_out[...] = vel[...]
    den_out[...] = den[...]
    ele_out[...] = ele[...]
    drift_out[...] = drift[:, :STEPS]


def solution(mesh):
    n_space, n_level = mesh.shape["space"], mesh.shape["level"]
    n_dev = n_space * n_level
    width = max(w for w in range(1, n_space + 1) if n_space % w == 0 and w * w <= n_space)

    def local(velocity, density, elevation, grad_weights, lap_weights, coriolis,
              node_area, thickness, send_list, neighbours, bottom):
        rows, nodes = density.shape
        blocks = nodes // LANES
        near_count = neighbours.shape[0]
        f32, i32 = jnp.float32, jnp.int32
        plane = (blocks, LANES)
        vmem = pl.BlockSpec(memory_space=pltpu.VMEM)
        hbm = pl.BlockSpec(memory_space=pltpu.HBM)
        dma = pltpu.SemaphoreType.DMA
        tile = (rows, LANES)
        pack = (8, LANES)
        arrays = [velocity, density, elevation.reshape(plane), grad_weights.transpose(1, 0, 2), lap_weights,
                  coriolis.reshape(plane), node_area.reshape(plane), thickness, send_list,
                  neighbours, bottom.reshape(plane)]
        arrays = [pltpu.with_memory_space_constraint(a, pltpu.HBM) for a in arrays]
        out = pl.pallas_call(
            functools.partial(kernel, n_space, n_level, width, rows, blocks, near_count),
            out_shape=(
                jax.ShapeDtypeStruct(velocity.shape, f32),
                jax.ShapeDtypeStruct(density.shape, f32),
                jax.ShapeDtypeStruct(plane, f32),
                jax.ShapeDtypeStruct((1, LANES), f32),
            ),
            in_specs=[hbm] * 11,
            out_specs=(vmem, vmem, vmem, vmem),
            scratch_shapes=[
                pltpu.VMEM((3, blocks) + tile, f32),
                pltpu.VMEM((blocks,) + pack, f32),
                pltpu.VMEM((blocks, near_count) + tile, i32),
                pltpu.VMEM((blocks, near_count) + tile, i32),
                pltpu.VMEM((blocks, near_count, 6) + tile, f32),
                pltpu.VMEM((blocks,) + pack, i32),
                pltpu.VMEM((blocks,) + pack, i32),
                pltpu.VMEM((blocks, 4) + pack, f32),
                pltpu.VMEM((blocks, 6) + tile, f32),
                pltpu.VMEM((blocks, 2) + pack, f32),
                pltpu.VMEM((blocks + 2,) + pack, f32),
                pltpu.VMEM(plane, f32),
                pltpu.VMEM((blocks,) + pack, f32),
                pltpu.VMEM((STEPS, 2, 3 * rows + 8, LANES), f32),
                pltpu.VMEM((STEPS, 2, 2, 1, LANES), f32),
                pltpu.VMEM((STEPS, 2, 3 * rows + 8, LANES), f32),
                pltpu.VMEM((STEPS, 2, n_level, 1, LANES), f32),
                pltpu.VMEM((STEPS + 1, 2) + plane, f32),
                pltpu.VMEM((STEPS + 1, n_level) + plane, f32),
                pltpu.VMEM(pack, f32),
                pltpu.VMEM((1, LANES), f32),
                pltpu.VMEM((n_dev, 1, LANES), f32),
                dma((STEPS, 2)), dma((STEPS, 2)),
                dma((STEPS, 2, n_level)), dma((STEPS, 2, n_level)),
                dma((STEPS + 1, n_level)), dma((STEPS + 1, n_level)),
                dma((n_dev,)), dma((n_dev,)),
                pltpu.SemaphoreType.REGULAR,
                dma((11,)),
                pltpu.SMEM(thickness.shape, f32),
            ] + [pltpu.VMEM(a.shape, a.dtype) for a in arrays[:7] + arrays[8:]],
            compiler_params=pltpu.CompilerParams(
                collective_id=0, has_side_effects=True, vmem_limit_bytes=16 * 2 ** 20),
        )(*arrays)
        out = pl.pallas_call(
            emit,
            out_shape=(
                jax.ShapeDtypeStruct(velocity.shape, f32),
                jax.ShapeDtypeStruct(density.shape, f32),
                jax.ShapeDtypeStruct(plane, f32),
                jax.ShapeDtypeStruct((1, STEPS), f32),
            ),
            in_specs=[vmem] * 4,
            out_specs=(vmem,) * 4,
            compiler_params=pltpu.CompilerParams(vmem_limit_bytes=2 ** 20),
        )(*out)
        return out[0], out[1], out[2].reshape(nodes), out[3].reshape(STEPS)

    return jax.shard_map(
        local,
        mesh=mesh,
        in_specs=(
            P(None, "level", "space"),
            P("level", "space"),
            P("space"),
            P(None, None, "space"),
            P(None, "space"),
            P("space"),
            P("space"),
            P("level"),
            P("space", None),
            P(None, "space"),
            P("space"),
        ),
        out_specs=(P(None, "level", "space"), P("level", "space"), P("space"), P()),
        check_vma=False,
    )
```

```python
import functools

import jax
import jax.numpy as jnp
from jax import lax
from jax.experimental import pallas as pl
from jax.experimental.pallas import tpu as pltpu
from jax.sharding import PartitionSpec as P

STEPS = 4
LANES = 128

time_step = 0.1
buoyancy = 0.5
drag_rate = 0.5


def lane_gather(values, lanes):
    return jnp.take_along_axis(values, lanes, axis=1, mode="promise_in_bounds")


def pick(tiles, lanes, masks):
    found = lane_gather(tiles[0], lanes)
    for tile, mask in zip(tiles[1:], masks):
        found = jnp.where(mask, lane_gather(tile, lanes), found)
    return found


def running_sum(values, rows, row_ids):
    shift = 1
    while shift < rows:
        moved = pltpu.roll(values, shift, 0)
        values = values + jnp.where(row_ids >= shift, moved, 0.0)
        shift *= 2
    return values


def spread_sum(values):
    shift = values.shape[0] // 2
    while shift:
        values = values + pltpu.roll(values, shift, 0)
        shift //= 2
    return values


def kernel(
    n_space, n_level, width, rows, blocks, near_count,
    vel, den, ele, grad, lap, cor, area, thick, send, near, bot,
    vel_out, den_out, ele_out, drift_out,
    own, eta, cor_of, bot_of, lanes_of, block_of, weight_of, pack_lanes, pack_block, pack_weight,
    flow_lanes, flow_block, flow_own, flow_halo,
    part, q_part, q_of, q_edge, q_sum, small, out, out_small, halo, halo_small, peer_out, peer,
    vol, vol_line, vol_all, adjoint, adjoint_in,
    main_send, main_recv, hs_send, hs_recv, peer_send, peer_recv, vol_send, vol_recv, adj_send, adj_recv, column_in,
    load_sem, thick_in, *loaded,
):
    sp = lax.axis_index("space")
    lv = lax.axis_index("level")
    n_dev = n_space * n_level
    dev = sp * n_level + lv
    has = (sp > 0, sp < n_space - 1)
    ends = (sp - 1, sp + 1)
    low = jnp.where(has[0], 1, 0)
    high = jnp.where(has[1], 1, 0)
    others = [lax.rem(lv + d, n_level) for d in range(1, n_level)]
    targets = blocks + 2

    barrier = pltpu.get_barrier_semaphore()

    mine, place = sp // width, lax.rem(sp, width)
    column = [(lax.rem(sp + d * width, n_space), lv) for d in range(1, n_space // width)]
    row = [(mine * width + lax.rem(place + d, width), lax.rem(lv + e, n_level))
           for d in range(width) for e in range(n_level) if d or e]
    for q, level in row + column:
        pl.semaphore_signal(barrier, inc=1, device_id={"space": q, "level": level})
    for side in range(2):
        @pl.when(has[side])
        def _():
            for q in [lv] + others:
                pl.semaphore_signal(barrier, inc=1, device_id={"space": ends[side], "level": q})

    loads = [
        pltpu.make_async_copy(ref, buffer, load_sem.at[i])
        for i, (ref, buffer) in enumerate(zip(
            (vel, den, ele, grad, lap, cor, area, thick, send, near, bot),
            loaded[:7] + (thick_in,) + loaded[7:]))
    ]
    for load in loads:
        load.start()

    row_ids = lax.broadcasted_iota(jnp.int32, (rows, LANES), 0)
    eight = lax.broadcasted_iota(jnp.int32, (8, LANES), 0)
    odd = jnp.bitwise_and(eight, 1) == 1
    lane_ids = lax.broadcasted_iota(jnp.int32, (1, LANES), 1)
    level_ids = row_ids + lv * rows

    def wide(row, count=rows):
        return jnp.broadcast_to(row, (count, LANES))

    for side in range(2):
        @pl.when(jnp.logical_not(has[side]))
        def _():
            halo[:, side] = jnp.zeros(halo.shape[:1] + halo.shape[2:], jnp.float32)
            halo_small[:, side] = jnp.zeros(halo_small.shape[:1] + halo_small.shape[2:], jnp.float32)
            adjoint_in[side] = jnp.zeros(adjoint_in.shape[1:], jnp.float32)

    for load in loads:
        load.wait()
    vel, den, ele, grad, lap, cor, area, send, near, bot = loaded

    thickness = jnp.zeros((rows, LANES), jnp.float32)
    for r in range(rows):
        thickness = jnp.where(row_ids == r, thick_in[r], thickness)

    def prepare(t, _):
        here = pl.ds(pl.multiple_of(t * LANES, LANES), LANES)
        bottom = wide(bot[pl.ds(t, 1), :])
        turn = wide(cor[pl.ds(t, 1), :])
        bot_of[t] = bottom
        cor_of[t] = turn
        wet = level_ids < bottom
        own[0, t] = jnp.where(wet, vel[0, :, here], 0.0)
        own[1, t] = jnp.where(wet, vel[1, :, here], 0.0)
        own[2, t] = den[:, here]
        eta[t] = jnp.where(lv == 0, wide(ele[pl.ds(t, 1), :], 8), 0.0)
        lane_pack = jnp.zeros((8, LANES), jnp.int32)
        block_pack = bottom[:8]
        packs = [jnp.zeros((8, LANES), jnp.float32) for _ in range(6)]
        packs[2] = turn[:8]
        flows = [[jnp.zeros((8, LANES), jnp.int32)] * 2 + [jnp.zeros((8, LANES), jnp.float32)] * 2
                 for _ in range(flow_own.shape[1])]
        for k in range(near_count):
            slot = wide(near[k:k + 1, here])
            block = lax.shift_right_logical(slot, 7)
            lanes = jnp.bitwise_and(slot, LANES - 1)
            inside = block < blocks
            outside = jnp.where(inside, 0, jnp.where(block == blocks, low, high)) > 0
            lanes_of[t, k] = lanes
            block_of[t, k] = block
            values = (wide(grad[k, 0:1, here]), wide(grad[k, 1:2, here]), wide(lap[k:k + 1, here]))
            picked = [jnp.where(mask, value, 0.0) for mask in (inside, outside) for value in values]
            for i in range(6):
                weight_of[t, k, i] = picked[i]
            mine = eight == k
            lane_pack = jnp.where(mine, lanes[:8], lane_pack)
            block_pack = jnp.where(mine, block[:8], block_pack)
            packs = [jnp.where(mine, value[:8], pack) for value, pack in zip(picked, packs)]
            flow = flows[k // 4]
            first = 2 * (k % 4)
            pair = jnp.logical_or(eight == first, eight == first + 1)
            flow[0] = jnp.where(pair, lanes[:8], flow[0])
            flow[1] = jnp.where(pair, block[:8], flow[1])
            flow[2] = jnp.where(pair, jnp.where(odd, picked[1][:8], picked[0][:8]), flow[2])
            flow[3] = jnp.where(pair, jnp.where(odd, picked[4][:8], picked[3][:8]), flow[3])
        pack_lanes[t] = lane_pack
        pack_block[t] = block_pack
        for i in range(6):
            pack_weight[t, i] = packs[i]
        for j in range(flow_own.shape[1]):
            flow_lanes[t, j], flow_block[t, j], flow_own[t, j], flow_halo[t, j] = flows[j]
        return 0

    lax.fori_loop(0, blocks, prepare, 0)
    wet_area = area[...] * jnp.where(bot[...] > 0, 1.0, 0.0)
    area[...] = wet_area
    count = jnp.where(lv == 0, 1.0, 0.0)
    vol[...] = jnp.where(eight == STEPS, wide(jnp.sum(wet_area, axis=0, keepdims=True), 8) * count, 0.0)

    def listed(side):
        slot = wide(send[:, side * LANES:(side + 1) * LANES])
        block = lax.shift_right_logical(slot, 7)
        return jnp.bitwise_and(slot, LANES - 1), [block == b for b in range(1, blocks)]

    def listed_tables():
        for side in range(2):
            t = blocks + side
            lanes, masks = listed(side)
            lanes, masks = lanes[:8], [mask[:8] for mask in masks]
            found_lanes = pick([pack_lanes[b] for b in range(blocks)], lanes, masks)
            found_block = pick([pack_block[b] for b in range(blocks)], lanes, masks)
            found = [pick([pack_weight[b, i] for b in range(blocks)], lanes, masks) for i in range(6)]
            pack_lanes[t] = found_lanes
            pack_block[t] = found_block
            for i in range(6):
                pack_weight[t, i] = found[i]
            bot_of[t] = wide(found_block[7:8])
            cor_of[t] = wide(found[2][7:8])
            for k in range(near_count):
                lanes_of[t, k] = wide(found_lanes[k:k + 1])
                block_of[t, k] = wide(found_block[k:k + 1])
                for i in range(6):
                    weight_of[t, k, i] = wide(found[i][k:k + 1])

    def version(q):
        return jnp.where(q > lv, 1, 0)

    def main_copy(s, side):
        return pltpu.make_async_remote_copy(
            src_ref=out.at[s, side], dst_ref=halo.at[s, 1 - side],
            send_sem=main_send.at[s, side], recv_sem=main_recv.at[s, 1 - side],
            device_id={"space": ends[side], "level": lv}, device_id_type=pl.DeviceIdType.MESH)

    def small_copy(s, side, q, slot):
        return pltpu.make_async_remote_copy(
            src_ref=out_small.at[s, side, version(q)], dst_ref=halo_small.at[s, 1 - side, slot],
            send_sem=hs_send.at[s, side, q], recv_sem=hs_recv.at[s, 1 - side, slot],
            device_id={"space": ends[side], "level": q}, device_id_type=pl.DeviceIdType.MESH)

    def adjoint_copy(side):
        return pltpu.make_async_remote_copy(
            src_ref=adjoint.at[side], dst_ref=adjoint_in.at[1 - side],
            send_sem=adj_send.at[side], recv_sem=adj_recv.at[1 - side],
            device_id={"space": ends[side], "level": lv}, device_id_type=pl.DeviceIdType.MESH)

    def peer_copy(s, q, slot):
        return pltpu.make_async_remote_copy(
            src_ref=peer_out.at[s, jnp.where(s < STEPS, version(q), 0)], dst_ref=peer.at[s, slot],
            send_sem=peer_send.at[s, q], recv_sem=peer_recv.at[s, slot],
            device_id={"space": sp, "level": q}, device_id_type=pl.DeviceIdType.MESH)

    def vol_copy(d):
        q = lax.rem(dev + d, n_dev)
        return pltpu.make_async_remote_copy(
            src_ref=vol_line, dst_ref=vol_all.at[d - 1], send_sem=vol_send, recv_sem=vol_recv,
            device_id={"space": q // n_level, "level": lax.rem(q, n_level)},
            device_id_type=pl.DeviceIdType.MESH)

    def vol_every():
        q = lax.rem(dev + 1, n_dev)
        return pltpu.make_async_remote_copy(
            src_ref=vol_all, dst_ref=vol_all, send_sem=vol_send, recv_sem=vol_recv,
            device_id={"space": q // n_level, "level": lax.rem(q, n_level)},
            device_id_type=pl.DeviceIdType.MESH)

    def dense(rho, level):
        return level + buoyancy * spread_sum(rho * thickness)

    def stage(s, side, fields, level, heavy):
        for g in range(3):
            own[g, blocks + side] = fields[g]
            out[s, side, g * rows:(g + 1) * rows] = fields[g]
        eta[blocks + side] = level
        out[s, side, 3 * rows:3 * rows + 8] = level
        out_small[s, side, 0] = level[:1]
        out_small[s, side, 1] = heavy[:1]

    def send_out(s):
        for side in range(2):
            @pl.when(has[side])
            def _():
                main_copy(s, side).start()
                for q in others:
                    small_copy(s, side, q, lv).start()

    def close(s):
        for q in others:
            peer_copy(s, q, lv).wait_send()
        for side in range(2):
            @pl.when(has[side])
            def _():
                main_copy(s, side).wait_send()
                for q in others:
                    small_copy(s, side, q, lv).wait_send()

    def gathered(sums, diff, weights):
        east, north, smooth = weights
        return [sums[0] + smooth * diff[0], sums[1] + smooth * diff[1], sums[2] + smooth * diff[2],
                sums[3] + east * diff[2], sums[4] + north * diff[2],
                sums[5] + (east * diff[0] + north * diff[1])]

    def own_parts():
        def body(t, _):
            tiles = [[own[g, b] for b in range(blocks)] for g in range(3)]
            here = [own[g, t] for g in range(3)]
            zero = jnp.zeros((rows, LANES), jnp.float32)
            sums = [zero] * 6
            for k in range(near_count):
                block = block_of[t, k]
                masks = [block == b for b in range(1, blocks)]
                diff = [pick(tiles[g], lanes_of[t, k], masks) - here[g] for g in range(3)]
                sums = gathered(sums, diff, [weight_of[t, k, i] for i in range(3)])
            for i in range(6):
                part[t, i] = sums[i]
            return 0
        lax.fori_loop(0, targets, body, 0)

    def own_surface(s):
        total = peer_out[s, 0]
        for q in others:
            total = total + peer[s, q]
        q_sum[...] = total
        tiles = [wide(q_sum[t:t + 1, :], 8) for t in range(blocks)]
        for side in range(2):
            lanes, masks = listed(side)
            tiles.append(pick(tiles[:blocks], lanes[:8], [mask[:8] for mask in masks]))
        for t in range(targets):
            q_of[t] = tiles[t]
            block = pack_block[t]
            diff = pick(tiles[:blocks], pack_lanes[t], [block == b for b in range(1, blocks)]) - tiles[t]
            q_part[t, 0] = pack_weight[t, 0] * diff
            q_part[t, 1] = pack_weight[t, 1] * diff

    def receive(s):
        for side in range(2):
            @pl.when(has[side])
            def _():
                main_copy(s, 1 - side).wait_recv()
                for q in others:
                    small_copy(s, 1 - side, q, q).wait_recv()
        for side in range(2):
            total = halo[s, side, 3 * rows:3 * rows + 1]
            for q in others:
                total = total + halo_small[s, side, q]
            q_edge[side] = wide(total, 8)

    def advance(s, t):
        edges = [[halo[s, side, g * rows:(g + 1) * rows] for side in range(2)] for g in range(3)]
        here = [own[g, t] for g in range(3)]
        sums = [part[t, i] for i in range(6)]
        for k in range(near_count):
            lanes = lanes_of[t, k]
            upper = block_of[t, k] == blocks + 1
            diff = [jnp.where(upper, lane_gather(edges[g][1], lanes), lane_gather(edges[g][0], lanes)) - here[g]
                    for g in range(3)]
            sums = gathered(sums, diff, [weight_of[t, k, 3 + i] for i in range(3)])
        lap0, lap1, lap2, east2, north2, flow = sums
        lanes = pack_lanes[t]
        diff = jnp.where(pack_block[t] == blocks + 1, lane_gather(q_edge[1], lanes),
                         lane_gather(q_edge[0], lanes)) - q_of[t]
        slope0 = spread_sum(q_part[t, 0] + pack_weight[t, 3] * diff)
        slope1 = spread_sum(q_part[t, 1] + pack_weight[t, 4] * diff)
        bottom, turn = bot_of[t], cor_of[t]
        drag = jnp.where(level_ids == bottom - 1, drag_rate, 0.0)
        u, v, rho = here
        east3, north3 = thickness * east2, thickness * north2
        east3 = slope0 + buoyancy * (running_sum(east3, rows, row_ids) - 0.5 * east3)
        north3 = slope1 + buoyancy * (running_sum(north3, rows, row_ids) - 0.5 * north3)
        push0 = -east3 + turn * v + lap0 - drag * u
        push1 = -north3 - turn * u + lap1 - drag * v
        wet = level_ids < bottom
        fields = (jnp.where(wet, u + time_step * push0, 0.0), jnp.where(wet, v + time_step * push1, 0.0),
                  rho + time_step * (lap2 - u * east2 - v * north2))
        diverge = spread_sum(thickness * flow)
        level = eta[t] - time_step * jnp.where(bottom[:8] > 0, diverge, 0.0)
        return fields, diverge, level, dense(fields[2], level)

    def finish_listed(s):
        for side in range(2):
            fields, _, level, heavy = advance(s, blocks + side)
            stage(s + 1, side, fields, level, heavy)

    def finish(s):
        def body(t, carry):
            volume, light, heavy = carry
            fields, diverge, level, more = advance(s, t)
            for g in range(3):
                own[g, t] = fields[g]
            eta[t] = level
            return (volume + wide(area[pl.ds(t, 1), :], 8) * diverge,
                    jnp.where(eight == t, level, light), jnp.where(eight == t, more, heavy))

        zero = jnp.zeros((8, LANES), jnp.float32)
        volume, light, heavy = lax.fori_loop(0, blocks, body, (zero, zero, zero), unroll=True)
        vol[...] = jnp.where(eight == s, volume, vol[...])
        peer_out[s + 1, 0] = light
        peer_out[s + 1, 1] = heavy

    def make_adjoint():
        ids = lax.broadcasted_iota(jnp.int32, (2 * LANES, LANES), 0) + blocks * LANES

        def body(t, total):
            weight = wide(area[pl.ds(t, 1), :], 8)
            for k in range(near_count):
                slot = block_of[t, k][:1] * LANES + lanes_of[t, k][:1]
                hot = jnp.where(ids == jnp.broadcast_to(slot, ids.shape), 1.0, 0.0).astype(jnp.bfloat16)
                value = jnp.where(odd, weight_of[t, k, 4][:8], weight_of[t, k, 3][:8]) * weight
                high = value.astype(jnp.bfloat16).astype(jnp.float32)
                value = value - high
                middle = value.astype(jnp.bfloat16).astype(jnp.float32)
                value = value - middle
                value = jnp.where(eight < 2, high, jnp.where(eight < 4, middle, jnp.where(eight < 6, value, 0.0)))
                total = total + lax.dot_general(
                    value.astype(jnp.bfloat16), hot, (((1,), (1,)), ((), ())), preferred_element_type=jnp.float32)
            return total

        total = lax.fori_loop(0, blocks, body, jnp.zeros((8, 2 * LANES), jnp.float32))
        total = total + pltpu.roll(total, 4, 0)
        total = total + pltpu.roll(total, 2, 0)
        for side in range(2):
            adjoint[side] = total[:, side * LANES:(side + 1) * LANES]
            @pl.when(has[side])
            def _():
                adjoint_copy(side).start()

    def transport(t):
        return jnp.where(odd, spread_sum(thickness * own[1, t])[:8], spread_sum(thickness * own[0, t])[:8])

    def start_volume():
        for side in range(2):
            @pl.when(has[side])
            def _():
                adjoint_copy(1 - side).wait_recv()
        tiles = [transport(t) for t in range(blocks)]
        volume = jnp.zeros((8, LANES), jnp.float32)
        for t in range(blocks):
            total = jnp.zeros((8, LANES), jnp.float32)
            for j in range(flow_own.shape[1]):
                block = flow_block[t, j]
                found = pick(tiles, flow_lanes[t, j], [block == b for b in range(1, blocks)])
                total = total + (flow_own[t, j] * (found - tiles[t]) - flow_halo[t, j] * tiles[t])
            volume = volume + wide(area[t:t + 1, :], 8) * total
        for side in range(2):
            volume = volume + jnp.where(eight < 2, adjoint_in[side] * transport(blocks + side), 0.0)
        sums = jnp.sum(jnp.where(eight == STEPS - 1, spread_sum(volume), vol[...]), axis=1, keepdims=True)
        line = jnp.zeros((1, LANES), jnp.float32)
        for i in range(STEPS + 1):
            line = jnp.where(lane_ids == i, sums[i:i + 1], line)
        vol_line[...] = line
        pl.semaphore_wait(column_in, len(row))

        def start(d, _):
            vol_copy(d).start()
            return 0

        lax.fori_loop(1, n_dev, start, 0)

    def first(t, carry):
        light, heavy = carry
        more = dense(own[2, t], eta[t])
        small[t] = jnp.where(odd, more, eta[t])
        return jnp.where(eight == t, eta[t], light), jnp.where(eight == t, more, heavy)

    zero = jnp.zeros((8, LANES), jnp.float32)
    light, heavy = lax.fori_loop(0, blocks, first, (zero, zero), unroll=True)
    peer_out[0, 0] = light
    peer_out[0, 1] = heavy
    for side in range(2):
        lanes, masks = listed(side)
        fields = [pick([own[g, b] for b in range(blocks)], lanes, masks) for g in range(3)]
        found = pick([small[b] for b in range(blocks)], lanes[:8], [m[:8] for m in masks])
        stage(0, side, fields, wide(found[:1], 8), wide(found[1:2], 8))

    expected = len(row) + len(column) + n_level * (low + high)
    pl.semaphore_wait(barrier, expected)
    send_out(0)
    for q in others:
        peer_copy(0, q, lv).start()
    for q, level in row:
        pl.semaphore_signal(column_in, inc=1, device_id={"space": q, "level": level})
    listed_tables()

    def step(s, _):
        @pl.when(s == STEPS - 1)
        def _():
            start_volume()

        own_parts()

        @pl.when(s == 0)
        def _():
            make_adjoint()

        for q in others:
            peer_copy(s, q, q).wait_recv()
        own_surface(s)
        receive(s)

        @pl.when(s < STEPS - 1)
        def _():
            finish_listed(s)
            send_out(s + 1)

        finish(s)
        for q in others:
            peer_copy(s + 1, q, lv).start()
        close(s)
        return 0

    lax.fori_loop(0, STEPS, step, 0)

    for t in range(blocks):
        here = slice(t * LANES, (t + 1) * LANES)
        vel_out[0, :, here] = own[0, t]
        vel_out[1, :, here] = own[1, t]
        den_out[:, here] = own[2, t]

    level = peer_out[STEPS, 0]
    for q in others:
        peer_copy(STEPS, q, q).wait_recv()
        level = level + peer[STEPS, q]
    for q in others:
        peer_copy(STEPS, q, lv).wait_send()
    for side in range(2):
        @pl.when(has[side])
        def _():
            adjoint_copy(side).wait_send()

    vol_every().wait_send()
    vol_every().wait_recv()
    total = lax.fori_loop(0, n_dev - 1, lambda d, total: total + vol_all[d], vol_line[...], unroll=n_dev <= 64)
    drifts = total / total[:, STEPS:STEPS + 1]
    shift = jnp.sum(jnp.where(lane_ids < STEPS, drifts, 0.0), axis=1, keepdims=True)
    ele_out[...] = level + time_step * shift
    drift_out[...] = drifts


def emit(vel, den, ele, drift, vel_out, den_out, ele_out, drift_out):
    vel_out[...] = vel[...]
    den_out[...] = den[...]
    ele_out[...] = ele[...]
    drift_out[...] = drift[:, :STEPS]


def solution(mesh):
    n_space, n_level = mesh.shape["space"], mesh.shape["level"]
    n_dev = n_space * n_level
    width = max(w for w in range(1, n_space + 1) if n_space % w == 0 and w * w <= n_space)

    def local(velocity, density, elevation, grad_weights, lap_weights, coriolis,
              node_area, thickness, send_list, neighbours, bottom):
        rows, nodes = density.shape
        blocks = nodes // LANES
        near_count = neighbours.shape[0]
        assert near_count < 8 and rows == 8
        packs = -(-near_count // 4)
        f32, i32 = jnp.float32, jnp.int32
        plane = (blocks, LANES)
        vmem = pl.BlockSpec(memory_space=pltpu.VMEM)
        hbm = pl.BlockSpec(memory_space=pltpu.HBM)
        dma = pltpu.SemaphoreType.DMA
        tile = (rows, LANES)
        pack = (8, LANES)
        arrays = [velocity, density, elevation.reshape(plane), grad_weights.transpose(1, 0, 2), lap_weights,
                  coriolis.reshape(plane), node_area.reshape(plane), thickness, send_list,
                  neighbours, bottom.reshape(plane)]
        arrays = [pltpu.with_memory_space_constraint(a, pltpu.HBM) for a in arrays]
        out = pl.pallas_call(
            functools.partial(kernel, n_space, n_level, width, rows, blocks, near_count),
            out_shape=(
                jax.ShapeDtypeStruct(velocity.shape, f32),
                jax.ShapeDtypeStruct(density.shape, f32),
                jax.ShapeDtypeStruct(plane, f32),
                jax.ShapeDtypeStruct((1, LANES), f32),
            ),
            in_specs=[hbm] * 11,
            out_specs=(vmem, vmem, vmem, vmem),
            scratch_shapes=[
                pltpu.VMEM((3, blocks + 2) + tile, f32),
                pltpu.VMEM((blocks + 2,) + pack, f32),
                pltpu.VMEM((blocks + 2,) + tile, f32),
                pltpu.VMEM((blocks + 2,) + tile, i32),
                pltpu.VMEM((blocks + 2, near_count) + tile, i32),
                pltpu.VMEM((blocks + 2, near_count) + tile, i32),
                pltpu.VMEM((blocks + 2, near_count, 6) + tile, f32),
                pltpu.VMEM((blocks + 2,) + pack, i32),
                pltpu.VMEM((blocks + 2,) + pack, i32),
                pltpu.VMEM((blocks + 2, 6) + pack, f32),
                pltpu.VMEM((blocks, packs) + pack, i32),
                pltpu.VMEM((blocks, packs) + pack, i32),
                pltpu.VMEM((blocks, packs) + pack, f32),
                pltpu.VMEM((blocks, packs) + pack, f32),
                pltpu.VMEM((blocks + 2, 6) + tile, f32),
                pltpu.VMEM((blocks + 2, 2) + pack, f32),
                pltpu.VMEM((blocks + 2,) + pack, f32),
                pltpu.VMEM((2,) + pack, f32),
                pltpu.VMEM(plane, f32),
                pltpu.VMEM((blocks,) + pack, f32),
                pltpu.VMEM((STEPS, 2, 3 * rows + 8, LANES), f32),
                pltpu.VMEM((STEPS, 2, 2, 1, LANES), f32),
                pltpu.VMEM((STEPS, 2, 3 * rows + 8, LANES), f32),
                pltpu.VMEM((STEPS, 2, n_level, 1, LANES), f32),
                pltpu.VMEM((STEPS + 1, 2) + plane, f32),
                pltpu.VMEM((STEPS + 1, n_level) + plane, f32),
                pltpu.VMEM(pack, f32),
                pltpu.VMEM((1, LANES), f32),
                pltpu.VMEM((n_dev - 1, 1, LANES), f32),
                pltpu.VMEM((2,) + pack, f32),
                pltpu.VMEM((2,) + pack, f32),
                dma((STEPS, 2)), dma((STEPS, 2)),
                dma((STEPS, 2, n_level)), dma((STEPS, 2, n_level)),
                dma((STEPS + 1, n_level)), dma((STEPS + 1, n_level)),
                dma, dma,
                dma((2,)), dma((2,)),
                pltpu.SemaphoreType.REGULAR,
                dma((11,)),
                pltpu.SMEM(thickness.shape, f32),
            ] + [pltpu.VMEM(a.shape, a.dtype) for a in arrays[:7] + arrays[8:]],
            compiler_params=pltpu.CompilerParams(
                collective_id=0, has_side_effects=True, vmem_limit_bytes=16 * 2 ** 20),
        )(*arrays)
        out = pl.pallas_call(
            emit,
            out_shape=(
                jax.ShapeDtypeStruct(velocity.shape, f32),
                jax.ShapeDtypeStruct(density.shape, f32),
                jax.ShapeDtypeStruct(plane, f32),
                jax.ShapeDtypeStruct((1, STEPS), f32),
            ),
            in_specs=[vmem] * 4,
            out_specs=(vmem,) * 4,
            compiler_params=pltpu.CompilerParams(vmem_limit_bytes=2 ** 20),
        )(*out)
        return out[0], out[1], out[2].reshape(nodes), out[3].reshape(STEPS)

    return jax.shard_map(
        local,
        mesh=mesh,
        in_specs=(
            P(None, "level", "space"),
            P("level", "space"),
            P("space"),
            P(None, None, "space"),
            P(None, "space"),
            P("space"),
            P("space"),
            P("level"),
            P("space", None),
            P(None, "space"),
            P("space"),
        ),
        out_specs=(P(None, "level", "space"), P("level", "space"), P("space"), P()),
        check_vma=False,
    )
```

```python
import functools

import jax
import jax.numpy as jnp
from jax import lax
from jax.experimental import pallas as pl
from jax.experimental.pallas import tpu as pltpu
from jax.sharding import PartitionSpec as P

STEPS = 4
LANES = 128

time_step = 0.1
buoyancy = 0.5
drag_rate = 0.5


def lane_gather(values, lanes):
    return jnp.take_along_axis(values, lanes, axis=1, mode="promise_in_bounds")


def pick(tiles, lanes, masks):
    found = lane_gather(tiles[0], lanes)
    for tile, mask in zip(tiles[1:], masks):
        found = jnp.where(mask, lane_gather(tile, lanes), found)
    return found


def running_sum(values, rows, row_ids):
    shift = 1
    while shift < rows:
        moved = pltpu.roll(values, shift, 0)
        values = values + jnp.where(row_ids >= shift, moved, 0.0)
        shift *= 2
    return values


def spread_sum(values):
    shift = values.shape[0] // 2
    while shift:
        values = values + pltpu.roll(values, shift, 0)
        shift //= 2
    return values


def kernel(
    n_space, n_level, width, rows, blocks, near_count,
    vel, den, ele, grad, lap, cor, area, thick, send, near, bot,
    vel_out, den_out, ele_out, drift_out,
    own, eta, cor_of, bot_of, lanes_of, block_of, weight_of, pack_lanes, pack_block, pack_weight,
    flow_lanes, flow_block, flow_own, flow_halo,
    part, q_part, q_of, q_edge, q_sum, small, out, out_small, halo, halo_small, peer_out, peer,
    vol, vol_line, vol_all, adjoint_sum, adjoint, adjoint_in,
    main_send, main_recv, hs_send, hs_recv, peer_send, peer_recv, vol_send, vol_recv, adj_send, adj_recv, column_in,
    load_sem, thick_in, *loaded,
):
    sp = lax.axis_index("space")
    lv = lax.axis_index("level")
    n_dev = n_space * n_level
    dev = sp * n_level + lv
    has = (sp > 0, sp < n_space - 1)
    ends = (sp - 1, sp + 1)
    low = jnp.where(has[0], 1, 0)
    high = jnp.where(has[1], 1, 0)
    others = [lax.rem(lv + d, n_level) for d in range(1, n_level)]
    targets = blocks + 2

    barrier = pltpu.get_barrier_semaphore()

    mine, place = sp // width, lax.rem(sp, width)
    column = [(lax.rem(sp + d * width, n_space), lv) for d in range(1, n_space // width)]
    row = [(mine * width + lax.rem(place + d, width), lax.rem(lv + e, n_level))
           for d in range(width) for e in range(n_level) if d or e]
    for q, level in row + column:
        pl.semaphore_signal(barrier, inc=1, device_id={"space": q, "level": level})
    for side in range(2):
        @pl.when(has[side])
        def _():
            for q in [lv] + others:
                pl.semaphore_signal(barrier, inc=1, device_id={"space": ends[side], "level": q})

    loads = [
        pltpu.make_async_copy(ref, buffer, load_sem.at[i])
        for i, (ref, buffer) in enumerate(zip(
            (vel, den, ele, grad, lap, cor, area, thick, send, near, bot),
            loaded[:7] + (thick_in,) + loaded[7:]))
    ]
    for load in loads:
        load.start()

    row_ids = lax.broadcasted_iota(jnp.int32, (rows, LANES), 0)
    eight = lax.broadcasted_iota(jnp.int32, (8, LANES), 0)
    odd = jnp.bitwise_and(eight, 1) == 1
    lane_ids = lax.broadcasted_iota(jnp.int32, (1, LANES), 1)
    level_ids = row_ids + lv * rows

    def wide(row, count=rows):
        return jnp.broadcast_to(row, (count, LANES))

    for side in range(2):
        @pl.when(jnp.logical_not(has[side]))
        def _():
            halo[:, side] = jnp.zeros(halo.shape[:1] + halo.shape[2:], jnp.float32)
            halo_small[:, side] = jnp.zeros(halo_small.shape[:1] + halo_small.shape[2:], jnp.float32)
            adjoint_in[side] = jnp.zeros(adjoint_in.shape[1:], jnp.float32)

    early = (0, 1, 2, 7, 8, 10)
    for i in early:
        loads[i].wait()
    vel, den, ele, grad, lap, cor, area, send, near, bot = loaded

    thickness = jnp.zeros((rows, LANES), jnp.float32)
    for r in range(rows):
        thickness = jnp.where(row_ids == r, thick_in[r], thickness)

    def prepare(t, _):
        here = pl.ds(pl.multiple_of(t * LANES, LANES), LANES)
        bottom = bot_of[t]
        turn = wide(cor[pl.ds(t, 1), :])
        cor_of[t] = turn
        lane_pack = jnp.zeros((8, LANES), jnp.int32)
        block_pack = bottom[:8]
        packs = [jnp.zeros((8, LANES), jnp.float32) for _ in range(6)]
        packs[2] = turn[:8]
        flows = [[jnp.zeros((8, LANES), jnp.int32)] * 2 + [jnp.zeros((8, LANES), jnp.float32)] * 2
                 for _ in range(flow_own.shape[1])]
        for k in range(near_count):
            slot = wide(near[k:k + 1, here])
            block = lax.shift_right_logical(slot, 7)
            lanes = jnp.bitwise_and(slot, LANES - 1)
            inside = block < blocks
            outside = jnp.where(inside, 0, jnp.where(block == blocks, low, high)) > 0
            lanes_of[t, k] = lanes
            block_of[t, k] = block
            values = (wide(grad[k, 0:1, here]), wide(grad[k, 1:2, here]), wide(lap[k:k + 1, here]))
            picked = [jnp.where(mask, value, 0.0) for mask in (inside, outside) for value in values]
            for i in range(6):
                weight_of[t, k, i] = picked[i]
            mine = eight == k
            lane_pack = jnp.where(mine, lanes[:8], lane_pack)
            block_pack = jnp.where(mine, block[:8], block_pack)
            packs = [jnp.where(mine, value[:8], pack) for value, pack in zip(picked, packs)]
            flow = flows[k // 4]
            first = 2 * (k % 4)
            pair = jnp.logical_or(eight == first, eight == first + 1)
            flow[0] = jnp.where(pair, lanes[:8], flow[0])
            flow[1] = jnp.where(pair, block[:8], flow[1])
            flow[2] = jnp.where(pair, jnp.where(odd, picked[1][:8], picked[0][:8]), flow[2])
            flow[3] = jnp.where(pair, jnp.where(odd, picked[4][:8], picked[3][:8]), flow[3])
        pack_lanes[t] = lane_pack
        pack_block[t] = block_pack
        for i in range(6):
            pack_weight[t, i] = packs[i]
        for j in range(flow_own.shape[1]):
            flow_lanes[t, j], flow_block[t, j], flow_own[t, j], flow_halo[t, j] = flows[j]
        return 0


    def listed(side):
        slot = wide(send[:, side * LANES:(side + 1) * LANES])
        block = lax.shift_right_logical(slot, 7)
        return jnp.bitwise_and(slot, LANES - 1), [block == b for b in range(1, blocks)]

    def listed_tables():
        for side in range(2):
            t = blocks + side
            lanes, masks = listed(side)
            lanes, masks = lanes[:8], [mask[:8] for mask in masks]
            found_lanes = pick([pack_lanes[b] for b in range(blocks)], lanes, masks)
            found_block = pick([pack_block[b] for b in range(blocks)], lanes, masks)
            found = [pick([pack_weight[b, i] for b in range(blocks)], lanes, masks) for i in range(6)]
            pack_lanes[t] = found_lanes
            pack_block[t] = found_block
            for i in range(6):
                pack_weight[t, i] = found[i]
            bot_of[t] = wide(found_block[7:8])
            cor_of[t] = wide(found[2][7:8])
            for k in range(near_count):
                lanes_of[t, k] = wide(found_lanes[k:k + 1])
                block_of[t, k] = wide(found_block[k:k + 1])
                for i in range(6):
                    weight_of[t, k, i] = wide(found[i][k:k + 1])

    def version(q):
        return jnp.where(q > lv, 1, 0)

    def main_copy(s, side):
        return pltpu.make_async_remote_copy(
            src_ref=out.at[s, side], dst_ref=halo.at[s, 1 - side],
            send_sem=main_send.at[side], recv_sem=main_recv.at[lax.rem(s, 2), 1 - side],
            device_id={"space": ends[side], "level": lv}, device_id_type=pl.DeviceIdType.MESH)

    def small_copy(s, side, q, slot):
        return pltpu.make_async_remote_copy(
            src_ref=out_small.at[s, side, version(q)], dst_ref=halo_small.at[s, 1 - side, slot],
            send_sem=hs_send.at[side, q], recv_sem=hs_recv.at[lax.rem(s, 2), 1 - side, slot],
            device_id={"space": ends[side], "level": q}, device_id_type=pl.DeviceIdType.MESH)

    def adjoint_copy(side):
        return pltpu.make_async_remote_copy(
            src_ref=adjoint.at[side], dst_ref=adjoint_in.at[1 - side],
            send_sem=adj_send.at[side], recv_sem=adj_recv.at[1 - side],
            device_id={"space": ends[side], "level": lv}, device_id_type=pl.DeviceIdType.MESH)

    def peer_copy(s, q, slot):
        return pltpu.make_async_remote_copy(
            src_ref=peer_out.at[s, jnp.where(s < STEPS, version(q), 0)], dst_ref=peer.at[s, slot],
            send_sem=peer_send.at[q], recv_sem=peer_recv.at[lax.rem(s, 2), slot],
            device_id={"space": sp, "level": q}, device_id_type=pl.DeviceIdType.MESH)

    bits = n_dev.bit_length() - 1
    mirror = n_dev == 1 << bits and n_dev <= 64
    flips = [(1 - 2 * lax.rem(dev // (1 << i), 2)) * (1 << i) for i in range(bits)] if mirror else []

    def vol_copy(d):
        if mirror:
            q = dev + sum(flips[i] for i in range(bits) if d >> i & 1)
        else:
            q = lax.rem(dev + d, n_dev)
        return pltpu.make_async_remote_copy(
            src_ref=vol_line, dst_ref=vol_all.at[d - 1], send_sem=vol_send, recv_sem=vol_recv,
            device_id={"space": q // n_level, "level": lax.rem(q, n_level)},
            device_id_type=pl.DeviceIdType.MESH)

    def vol_every():
        q = lax.rem(dev + 1, n_dev)
        return pltpu.make_async_remote_copy(
            src_ref=vol_all, dst_ref=vol_all, send_sem=vol_send, recv_sem=vol_recv,
            device_id={"space": q // n_level, "level": lax.rem(q, n_level)},
            device_id_type=pl.DeviceIdType.MESH)

    def dense(rho, level):
        return level + buoyancy * spread_sum(rho * thickness)

    def stage(s, side, fields, level, heavy):
        for g in range(3):
            own[g, blocks + side] = fields[g]
            out[s, side, g * rows:(g + 1) * rows] = fields[g]
        eta[blocks + side] = level
        out[s, side, 3 * rows:3 * rows + 8] = level
        out_small[s, side, 0] = level[:1]
        out_small[s, side, 1] = heavy[:1]

    def send_out(s):
        for side in range(2):
            @pl.when(has[side])
            def _():
                main_copy(s, side).start()
                for q in others:
                    small_copy(s, side, q, lv).start()

    def close(s):
        for q in others:
            peer_copy(s, q, lv).wait_send()
        for side in range(2):
            @pl.when(has[side])
            def _():
                main_copy(s, side).wait_send()
                for q in others:
                    small_copy(s, side, q, lv).wait_send()

    def gathered(sums, diff, weights):
        east, north, smooth = weights
        return [sums[0] + smooth * diff[0], sums[1] + smooth * diff[1], sums[2] + smooth * diff[2],
                sums[3] + east * diff[2], sums[4] + north * diff[2],
                sums[5] + (east * diff[0] + north * diff[1])]

    def own_parts():
        def body(t, _):
            tiles = [[own[g, b] for b in range(blocks)] for g in range(3)]
            here = [own[g, t] for g in range(3)]
            zero = jnp.zeros((rows, LANES), jnp.float32)
            sums = [zero] * 6
            for k in range(near_count):
                block = block_of[t, k]
                masks = [block == b for b in range(1, blocks)]
                diff = [pick(tiles[g], lanes_of[t, k], masks) - here[g] for g in range(3)]
                sums = gathered(sums, diff, [weight_of[t, k, i] for i in range(3)])
            for i in range(6):
                part[t, i] = sums[i]
            return 0
        several = max(d for d in (1, 2, 5) if targets % d == 0)

        def bodies(i, _):
            for j in range(several):
                body(i * several + j, 0)
            return 0
        lax.fori_loop(0, targets // several, bodies, 0)

    def own_surface(s):
        total = peer_out[s, 0]
        for q in others:
            total = total + peer[s, q]
        q_sum[...] = total
        tiles = [wide(q_sum[t:t + 1, :], 8) for t in range(blocks)]
        for side in range(2):
            lanes, masks = listed(side)
            tiles.append(pick(tiles[:blocks], lanes[:8], [mask[:8] for mask in masks]))
        for t in range(targets):
            q_of[t] = tiles[t]
            block = pack_block[t]
            diff = pick(tiles[:blocks], pack_lanes[t], [block == b for b in range(1, blocks)]) - tiles[t]
            q_part[t, 0] = pack_weight[t, 0] * diff
            q_part[t, 1] = pack_weight[t, 1] * diff

    def receive(s):
        for side in range(2):
            @pl.when(has[side])
            def _():
                main_copy(s, 1 - side).wait_recv()
                for q in others:
                    small_copy(s, 1 - side, q, q).wait_recv()
        for side in range(2):
            total = halo[s, side, 3 * rows:3 * rows + 1]
            for q in others:
                total = total + halo_small[s, side, q]
            q_edge[side] = wide(total, 8)

    def advance(s, t):
        edges = [[halo[s, side, g * rows:(g + 1) * rows] for side in range(2)] for g in range(3)]
        here = [own[g, t] for g in range(3)]
        sums = [part[t, i] for i in range(6)]
        for k in range(near_count):
            lanes = lanes_of[t, k]
            upper = block_of[t, k] == blocks + 1
            diff = [jnp.where(upper, lane_gather(edges[g][1], lanes), lane_gather(edges[g][0], lanes)) - here[g]
                    for g in range(3)]
            sums = gathered(sums, diff, [weight_of[t, k, 3 + i] for i in range(3)])
        lap0, lap1, lap2, east2, north2, flow = sums
        lanes = pack_lanes[t]
        diff = jnp.where(pack_block[t] == blocks + 1, lane_gather(q_edge[1], lanes),
                         lane_gather(q_edge[0], lanes)) - q_of[t]
        slope0 = spread_sum(q_part[t, 0] + pack_weight[t, 3] * diff)
        slope1 = spread_sum(q_part[t, 1] + pack_weight[t, 4] * diff)
        bottom, turn = bot_of[t], cor_of[t]
        drag = jnp.where(level_ids == bottom - 1, drag_rate, 0.0)
        u, v, rho = here
        east3, north3 = thickness * east2, thickness * north2
        east3 = slope0 + buoyancy * (running_sum(east3, rows, row_ids) - 0.5 * east3)
        north3 = slope1 + buoyancy * (running_sum(north3, rows, row_ids) - 0.5 * north3)
        push0 = -east3 + turn * v + lap0 - drag * u
        push1 = -north3 - turn * u + lap1 - drag * v
        wet = level_ids < bottom
        fields = (jnp.where(wet, u + time_step * push0, 0.0), jnp.where(wet, v + time_step * push1, 0.0),
                  rho + time_step * (lap2 - u * east2 - v * north2))
        diverge = spread_sum(thickness * flow)
        level = eta[t] - time_step * jnp.where(bottom[:8] > 0, diverge, 0.0)
        return fields, diverge, level, dense(fields[2], level)

    def finish_listed(s):
        for side in range(2):
            fields, _, level, heavy = advance(s, blocks + side)
            stage(s + 1, side, fields, level, heavy)

    def finish(s):
        def body(t, carry):
            volume, light, heavy = carry
            fields, diverge, level, more = advance(s, t)
            for g in range(3):
                own[g, t] = fields[g]
            eta[t] = level
            return (volume + wide(area[pl.ds(t, 1), :], 8) * diverge,
                    jnp.where(eight == t, level, light), jnp.where(eight == t, more, heavy))

        zero = jnp.zeros((8, LANES), jnp.float32)
        volume, light, heavy = lax.fori_loop(0, blocks, body, (zero, zero, zero), unroll=True)
        vol[...] = jnp.where(eight == s, volume, vol[...])
        peer_out[s + 1, 0] = light
        peer_out[s + 1, 1] = heavy

    def make_adjoint(s):
        ids = lax.broadcasted_iota(jnp.int32, (2 * LANES, LANES), 0) + blocks * LANES

        def body(t, total):
            weight = wide(area[pl.ds(t, 1), :], 8)
            for k in range(near_count):
                slot = block_of[t, k][:1] * LANES + lanes_of[t, k][:1]
                hot = jnp.where(ids == jnp.broadcast_to(slot, ids.shape), 1.0, 0.0).astype(jnp.bfloat16)
                value = jnp.where(odd, weight_of[t, k, 4][:8], weight_of[t, k, 3][:8]) * weight
                high = value.astype(jnp.bfloat16).astype(jnp.float32)
                value = value - high
                middle = value.astype(jnp.bfloat16).astype(jnp.float32)
                value = value - middle
                value = jnp.where(eight < 2, high, jnp.where(eight < 4, middle, jnp.where(eight < 6, value, 0.0)))
                total = total + lax.dot_general(
                    value.astype(jnp.bfloat16), hot, (((1,), (1,)), ((), ())), preferred_element_type=jnp.float32)
            return total

        half = -(-blocks // 2)
        total = lax.fori_loop(s * half, jnp.minimum((s + 1) * half, blocks), body, adjoint_sum[...])
        adjoint_sum[...] = total
        total = total + pltpu.roll(total, 4, 0)
        total = total + pltpu.roll(total, 2, 0)
        for side in range(2):
            adjoint[side] = total[:, side * LANES:(side + 1) * LANES]
            @pl.when(jnp.logical_and(has[side], s == 1))
            def _():
                adjoint_copy(side).start()

    def transport(t):
        return jnp.where(odd, spread_sum(thickness * own[1, t])[:8], spread_sum(thickness * own[0, t])[:8])

    def start_volume():
        for side in range(2):
            @pl.when(has[side])
            def _():
                adjoint_copy(1 - side).wait_recv()
        tiles = [transport(t) for t in range(blocks)]
        volume = jnp.zeros((8, LANES), jnp.float32)
        for t in range(blocks):
            total = jnp.zeros((8, LANES), jnp.float32)
            for j in range(flow_own.shape[1]):
                block = flow_block[t, j]
                found = pick(tiles, flow_lanes[t, j], [block == b for b in range(1, blocks)])
                total = total + (flow_own[t, j] * (found - tiles[t]) - flow_halo[t, j] * tiles[t])
            volume = volume + wide(area[t:t + 1, :], 8) * total
        for side in range(2):
            volume = volume + jnp.where(eight < 2, adjoint_in[side] * transport(blocks + side), 0.0)
        sums = jnp.sum(jnp.where(eight == STEPS - 1, spread_sum(volume), vol[...]), axis=1, keepdims=True)
        line = jnp.zeros((1, LANES), jnp.float32)
        for i in range(STEPS + 1):
            line = jnp.where(lane_ids == i, sums[i:i + 1], line)
        vol_line[...] = line
        pl.semaphore_wait(column_in, len(row))

        if mirror:
            for d in range(n_dev - 1, 0, -1):
                vol_copy(d).start()
        else:
            def start(d, _):
                vol_copy(d).start()
                return 0

            lax.fori_loop(1, n_dev, start, 0)

    def first(t, carry):
        light, heavy = carry
        here = slice(t * LANES, (t + 1) * LANES)
        bottom = wide(bot[t:t + 1, :])
        bot_of[t] = bottom
        wet = level_ids < bottom
        own[0, t] = jnp.where(wet, vel[0, :, here], 0.0)
        own[1, t] = jnp.where(wet, vel[1, :, here], 0.0)
        own[2, t] = den[:, here]
        level = jnp.where(lv == 0, wide(ele[t:t + 1, :], 8), 0.0)
        eta[t] = level
        more = dense(own[2, t], level)
        small[t] = jnp.where(odd, more, level)
        return jnp.where(eight == t, level, light), jnp.where(eight == t, more, heavy)

    zero = jnp.zeros((8, LANES), jnp.float32)
    light, heavy = zero, zero
    for t in range(blocks):
        light, heavy = first(t, (light, heavy))
    peer_out[0, 0] = light
    peer_out[0, 1] = heavy
    for side in range(2):
        lanes, masks = listed(side)
        fields = [pick([own[g, b] for b in range(blocks)], lanes, masks) for g in range(3)]
        found = pick([small[b] for b in range(blocks)], lanes[:8], [m[:8] for m in masks])
        stage(0, side, fields, wide(found[:1], 8), wide(found[1:2], 8))

    expected = len(row) + len(column) + n_level * (low + high)
    pl.semaphore_wait(barrier, expected)
    send_out(0)
    for q in others:
        peer_copy(0, q, lv).start()
    for q, level in row:
        pl.semaphore_signal(column_in, inc=1, device_id={"space": q, "level": level})
    for i in range(len(loads)):
        if i not in early:
            loads[i].wait()
    lax.fori_loop(0, blocks, prepare, 0)
    wet_area = area[...] * jnp.where(bot[...] > 0, 1.0, 0.0)
    area[...] = wet_area
    count = jnp.where(lv == 0, 1.0, 0.0)
    vol[...] = jnp.where(eight == STEPS, wide(jnp.sum(wet_area, axis=0, keepdims=True), 8) * count, 0.0)
    adjoint_sum[...] = jnp.zeros((8, 2 * LANES), jnp.float32)
    listed_tables()

    def step(s, _):
        @pl.when(s == STEPS - 1)
        def _():
            start_volume()

        own_parts()

        @pl.when(s < 2)
        def _():
            make_adjoint(s)

        for q in others:
            peer_copy(s, q, q).wait_recv()
        own_surface(s)
        receive(s)

        close(s)

        @pl.when(s < STEPS - 1)
        def _():
            finish_listed(s)
            send_out(s + 1)

        finish(s)
        for q in others:
            peer_copy(s + 1, q, lv).start()
        return 0

    lax.fori_loop(0, STEPS, step, 0)

    for t in range(blocks):
        here = slice(t * LANES, (t + 1) * LANES)
        vel_out[0, :, here] = own[0, t]
        vel_out[1, :, here] = own[1, t]
        den_out[:, here] = own[2, t]

    level = peer_out[STEPS, 0]
    for q in others:
        peer_copy(STEPS, q, q).wait_recv()
        level = level + peer[STEPS, q]
    for q in others:
        peer_copy(STEPS, q, lv).wait_send()
    for side in range(2):
        @pl.when(has[side])
        def _():
            adjoint_copy(side).wait_send()

    vol_every().wait_send()
    vol_every().wait_recv()
    total = lax.fori_loop(0, n_dev - 1, lambda d, total: total + vol_all[d], vol_line[...], unroll=n_dev <= 64)
    drifts = total / total[:, STEPS:STEPS + 1]
    shift = jnp.sum(jnp.where(lane_ids < STEPS, drifts, 0.0), axis=1, keepdims=True)
    ele_out[...] = level + time_step * shift
    drift_out[...] = drifts


def emit(vel, den, ele, drift, vel_out, den_out, ele_out, drift_out):
    vel_out[...] = vel[...]
    den_out[...] = den[...]
    ele_out[...] = ele[...]
    drift_out[...] = drift[:, :STEPS]


def solution(mesh):
    n_space, n_level = mesh.shape["space"], mesh.shape["level"]
    n_dev = n_space * n_level
    width = max(w for w in range(1, n_space + 1) if n_space % w == 0 and w * w <= n_space)

    def local(velocity, density, elevation, grad_weights, lap_weights, coriolis,
              node_area, thickness, send_list, neighbours, bottom):
        rows, nodes = density.shape
        blocks = nodes // LANES
        near_count = neighbours.shape[0]
        assert near_count < 8 and rows == 8
        packs = -(-near_count // 4)
        f32, i32 = jnp.float32, jnp.int32
        plane = (blocks, LANES)
        vmem = pl.BlockSpec(memory_space=pltpu.VMEM)
        hbm = pl.BlockSpec(memory_space=pltpu.HBM)
        dma = pltpu.SemaphoreType.DMA
        tile = (rows, LANES)
        pack = (8, LANES)
        arrays = [velocity, density, elevation.reshape(plane), grad_weights.transpose(1, 0, 2), lap_weights,
                  coriolis.reshape(plane), node_area.reshape(plane), thickness, send_list,
                  neighbours, bottom.reshape(plane)]
        arrays = [pltpu.with_memory_space_constraint(a, pltpu.HBM) for a in arrays]
        out = pl.pallas_call(
            functools.partial(kernel, n_space, n_level, width, rows, blocks, near_count),
            out_shape=(
                jax.ShapeDtypeStruct(velocity.shape, f32),
                jax.ShapeDtypeStruct(density.shape, f32),
                jax.ShapeDtypeStruct(plane, f32),
                jax.ShapeDtypeStruct((1, LANES), f32),
            ),
            in_specs=[hbm] * 11,
            out_specs=(vmem, vmem, vmem, vmem),
            scratch_shapes=[
                pltpu.VMEM((3, blocks + 2) + tile, f32),
                pltpu.VMEM((blocks + 2,) + pack, f32),
                pltpu.VMEM((blocks + 2,) + tile, f32),
                pltpu.VMEM((blocks + 2,) + tile, i32),
                pltpu.VMEM((blocks + 2, near_count) + tile, i32),
                pltpu.VMEM((blocks + 2, near_count) + tile, i32),
                pltpu.VMEM((blocks + 2, near_count, 6) + tile, f32),
                pltpu.VMEM((blocks + 2,) + pack, i32),
                pltpu.VMEM((blocks + 2,) + pack, i32),
                pltpu.VMEM((blocks + 2, 6) + pack, f32),
                pltpu.VMEM((blocks, packs) + pack, i32),
                pltpu.VMEM((blocks, packs) + pack, i32),
                pltpu.VMEM((blocks, packs) + pack, f32),
                pltpu.VMEM((blocks, packs) + pack, f32),
                pltpu.VMEM((blocks + 2, 6) + tile, f32),
                pltpu.VMEM((blocks + 2, 2) + pack, f32),
                pltpu.VMEM((blocks + 2,) + pack, f32),
                pltpu.VMEM((2,) + pack, f32),
                pltpu.VMEM(plane, f32),
                pltpu.VMEM((blocks,) + pack, f32),
                pltpu.VMEM((STEPS, 2, 3 * rows + 8, LANES), f32),
                pltpu.VMEM((STEPS, 2, 2, 1, LANES), f32),
                pltpu.VMEM((STEPS, 2, 3 * rows + 8, LANES), f32),
                pltpu.VMEM((STEPS, 2, n_level, 1, LANES), f32),
                pltpu.VMEM((STEPS + 1, 2) + plane, f32),
                pltpu.VMEM((STEPS + 1, n_level) + plane, f32),
                pltpu.VMEM(pack, f32),
                pltpu.VMEM((1, LANES), f32),
                pltpu.VMEM((n_dev - 1, 1, LANES), f32),
                pltpu.VMEM((8, 2 * LANES), f32),
                pltpu.VMEM((2,) + pack, f32),
                pltpu.VMEM((2,) + pack, f32),
                dma((2,)), dma((2, 2)),
                dma((2, n_level)), dma((2, 2, n_level)),
                dma((n_level,)), dma((2, n_level)),
                dma, dma,
                dma((2,)), dma((2,)),
                pltpu.SemaphoreType.REGULAR,
                dma((11,)),
                pltpu.SMEM(thickness.shape, f32),
            ] + [pltpu.VMEM(a.shape, a.dtype) for a in arrays[:7] + arrays[8:]],
            compiler_params=pltpu.CompilerParams(
                collective_id=0, has_side_effects=True, vmem_limit_bytes=16 * 2 ** 20),
        )(*arrays)
        out = pl.pallas_call(
            emit,
            out_shape=(
                jax.ShapeDtypeStruct(velocity.shape, f32),
                jax.ShapeDtypeStruct(density.shape, f32),
                jax.ShapeDtypeStruct(plane, f32),
                jax.ShapeDtypeStruct((1, STEPS), f32),
            ),
            in_specs=[vmem] * 4,
            out_specs=(vmem,) * 4,
            compiler_params=pltpu.CompilerParams(vmem_limit_bytes=2 ** 20),
        )(*out)
        return out[0], out[1], out[2].reshape(nodes), out[3].reshape(STEPS)

    return jax.shard_map(
        local,
        mesh=mesh,
        in_specs=(
            P(None, "level", "space"),
            P("level", "space"),
            P("space"),
            P(None, None, "space"),
            P(None, "space"),
            P("space"),
            P("space"),
            P("level"),
            P("space", None),
            P(None, "space"),
            P("space"),
        ),
        out_specs=(P(None, "level", "space"), P("level", "space"), P("space"), P()),
        check_vma=False,
    )
```

```python
import functools

import jax
import jax.numpy as jnp
from jax import lax
from jax.experimental import pallas as pl
from jax.experimental.pallas import tpu as pltpu
from jax.sharding import PartitionSpec as P

STEPS = 4
LANES = 128

time_step = 0.1
buoyancy = 0.5
drag_rate = 0.5


def lane_gather(values, lanes):
    return jnp.take_along_axis(values, lanes, axis=1, mode="promise_in_bounds")


def pick(tiles, lanes, masks):
    found = lane_gather(tiles[0], lanes)
    for tile, mask in zip(tiles[1:], masks):
        found = jnp.where(mask, lane_gather(tile, lanes), found)
    return found


def running_sum(values, rows, row_ids):
    shift = 1
    while shift < rows:
        moved = pltpu.roll(values, shift, 0)
        values = values + jnp.where(row_ids >= shift, moved, 0.0)
        shift *= 2
    return values


def spread_sum(values):
    shift = values.shape[0] // 2
    while shift:
        values = values + pltpu.roll(values, shift, 0)
        shift //= 2
    return values


def kernel(
    n_space, n_level, rows, blocks, near_count,
    vel, den, ele, grad, lap, cor, area, thick, send, near, bot,
    vel_out, den_out, ele_out, drift_out,
    own, eta, cor_of, bot_of, lanes_of, block_of, weight_of, pack_lanes, pack_block, pack_weight,
    flow_lanes, flow_block, flow_own, flow_halo,
    part, q_part, q_of, q_edge, q_sum, small, out, out_small, halo, halo_small, peer_out, peer,
    flow, vol, vol_line, line, lines, adjoint_sum, adjoint, adjoint_in,
    main_send, main_recv, hs_send, hs_recv, peer_send, peer_recv, line_send, line_recv, adj_send, adj_recv, ready,
    load_sem, thick_in, *loaded,
):
    sp = lax.axis_index("space")
    lv = lax.axis_index("level")
    n_dev = n_space * n_level
    dev = sp * n_level + lv
    has = (sp > 0, sp < n_space - 1)
    ends = (sp - 1, sp + 1)
    low = jnp.where(has[0], 1, 0)
    high = jnp.where(has[1], 1, 0)
    others = [lax.rem(lv + d, n_level) for d in range(1, n_level)]
    targets = blocks + 2

    barrier = pltpu.get_barrier_semaphore()

    for side in range(2):
        @pl.when(has[side])
        def _():
            for q in [lv] + others:
                pl.semaphore_signal(barrier, inc=1, device_id={"space": ends[side], "level": q})
    for q in others:
        pl.semaphore_signal(barrier, inc=1, device_id={"space": sp, "level": q})

    rounds = (n_space - 1).bit_length()

    def reached(j):
        return [(sp - (1 << j), sp >= 1 << j), (sp + (1 << j), sp + (1 << j) < n_space)]

    def tell(j):
        for q, there in reached(j):
            @pl.when(there)
            def _():
                pl.semaphore_signal(ready.at[j], inc=1, device_id={"space": q, "level": lv})

    def hear(j):
        pl.semaphore_wait(ready.at[j], sum(jnp.where(there, 1, 0) for _, there in reached(j)))

    loads = [
        pltpu.make_async_copy(ref, buffer, load_sem.at[i])
        for i, (ref, buffer) in enumerate(zip(
            (vel, den, ele, grad, lap, cor, area, thick, send, near, bot),
            loaded[:7] + (thick_in,) + loaded[7:]))
    ]
    for load in loads:
        load.start()

    row_ids = lax.broadcasted_iota(jnp.int32, (rows, LANES), 0)
    eight = lax.broadcasted_iota(jnp.int32, (8, LANES), 0)
    odd = jnp.bitwise_and(eight, 1) == 1
    lane_ids = lax.broadcasted_iota(jnp.int32, (1, LANES), 1)
    level_ids = row_ids + lv * rows

    def wide(row, count=rows):
        return jnp.broadcast_to(row, (count, LANES))

    for side in range(2):
        @pl.when(jnp.logical_not(has[side]))
        def _():
            halo[:, side] = jnp.zeros(halo.shape[:1] + halo.shape[2:], jnp.float32)
            halo_small[:, side] = jnp.zeros(halo_small.shape[:1] + halo_small.shape[2:], jnp.float32)
            adjoint_in[side] = jnp.zeros(adjoint_in.shape[1:], jnp.float32)

    early = (0, 1, 2, 7, 8, 10)
    for i in early:
        loads[i].wait()
    vel, den, ele, grad, lap, cor, area, send, near, bot = loaded

    thickness = jnp.zeros((rows, LANES), jnp.float32)
    for r in range(rows):
        thickness = jnp.where(row_ids == r, thick_in[r], thickness)

    def prepare(t, _):
        here = pl.ds(pl.multiple_of(t * LANES, LANES), LANES)
        bottom = bot_of[t]
        turn = wide(cor[pl.ds(t, 1), :])
        cor_of[t] = turn
        lane_pack = jnp.zeros((8, LANES), jnp.int32)
        block_pack = bottom[:8]
        packs = [jnp.zeros((8, LANES), jnp.float32) for _ in range(6)]
        packs[2] = turn[:8]
        flows = [[jnp.zeros((8, LANES), jnp.int32)] * 2 + [jnp.zeros((8, LANES), jnp.float32)] * 2
                 for _ in range(flow_own.shape[1])]
        for k in range(near_count):
            slot = wide(near[k:k + 1, here])
            block = lax.shift_right_logical(slot, 7)
            lanes = jnp.bitwise_and(slot, LANES - 1)
            inside = block < blocks
            outside = jnp.where(inside, 0, jnp.where(block == blocks, low, high)) > 0
            lanes_of[t, k] = lanes
            block_of[t, k] = block
            values = (wide(grad[k, 0:1, here]), wide(grad[k, 1:2, here]), wide(lap[k:k + 1, here]))
            picked = [jnp.where(mask, value, 0.0) for mask in (inside, outside) for value in values]
            for i in range(6):
                weight_of[t, k, i] = picked[i]
            mine = eight == k
            lane_pack = jnp.where(mine, lanes[:8], lane_pack)
            block_pack = jnp.where(mine, block[:8], block_pack)
            packs = [jnp.where(mine, value[:8], pack) for value, pack in zip(picked, packs)]
            flow = flows[k // 4]
            first = 2 * (k % 4)
            pair = jnp.logical_or(eight == first, eight == first + 1)
            flow[0] = jnp.where(pair, lanes[:8], flow[0])
            flow[1] = jnp.where(pair, block[:8], flow[1])
            flow[2] = jnp.where(pair, jnp.where(odd, picked[1][:8], picked[0][:8]), flow[2])
            flow[3] = jnp.where(pair, jnp.where(odd, picked[4][:8], picked[3][:8]), flow[3])
        pack_lanes[t] = lane_pack
        pack_block[t] = block_pack
        for i in range(6):
            pack_weight[t, i] = packs[i]
        for j in range(flow_own.shape[1]):
            flow_lanes[t, j], flow_block[t, j], flow_own[t, j], flow_halo[t, j] = flows[j]
        return 0


    def listed(side):
        slot = wide(send[:, side * LANES:(side + 1) * LANES])
        block = lax.shift_right_logical(slot, 7)
        return jnp.bitwise_and(slot, LANES - 1), [block == b for b in range(1, blocks)]

    def listed_tables():
        for side in range(2):
            t = blocks + side
            lanes, masks = listed(side)
            lanes, masks = lanes[:8], [mask[:8] for mask in masks]
            found_lanes = pick([pack_lanes[b] for b in range(blocks)], lanes, masks)
            found_block = pick([pack_block[b] for b in range(blocks)], lanes, masks)
            found = [pick([pack_weight[b, i] for b in range(blocks)], lanes, masks) for i in range(6)]
            pack_lanes[t] = found_lanes
            pack_block[t] = found_block
            for i in range(6):
                pack_weight[t, i] = found[i]
            bot_of[t] = wide(found_block[7:8])
            cor_of[t] = wide(found[2][7:8])
            for k in range(near_count):
                lanes_of[t, k] = wide(found_lanes[k:k + 1])
                block_of[t, k] = wide(found_block[k:k + 1])
                for i in range(6):
                    weight_of[t, k, i] = wide(found[i][k:k + 1])

    def version(q):
        return jnp.where(q > lv, 1, 0)

    def main_copy(s, side):
        return pltpu.make_async_remote_copy(
            src_ref=out.at[s, side], dst_ref=halo.at[s, 1 - side],
            send_sem=main_send.at[side], recv_sem=main_recv.at[lax.rem(s, 2), 1 - side],
            device_id={"space": ends[side], "level": lv}, device_id_type=pl.DeviceIdType.MESH)

    def small_copy(s, side, q, slot):
        return pltpu.make_async_remote_copy(
            src_ref=out_small.at[s, side, version(q)], dst_ref=halo_small.at[s, 1 - side, slot],
            send_sem=hs_send.at[side, q], recv_sem=hs_recv.at[lax.rem(s, 2), 1 - side, slot],
            device_id={"space": ends[side], "level": q}, device_id_type=pl.DeviceIdType.MESH)

    def adjoint_copy(side):
        return pltpu.make_async_remote_copy(
            src_ref=adjoint.at[side], dst_ref=adjoint_in.at[1 - side],
            send_sem=adj_send.at[side], recv_sem=adj_recv.at[1 - side],
            device_id={"space": ends[side], "level": lv}, device_id_type=pl.DeviceIdType.MESH)

    def peer_copy(s, q, slot):
        return pltpu.make_async_remote_copy(
            src_ref=peer_out.at[s, jnp.where(s < STEPS, version(q), 0)], dst_ref=peer.at[s, slot],
            send_sem=peer_send.at[q], recv_sem=peer_recv.at[lax.rem(s, 2), slot],
            device_id={"space": sp, "level": q}, device_id_type=pl.DeviceIdType.MESH)

    bits = n_dev.bit_length() - 1
    mirror = n_dev == 1 << bits and n_level == 1 << (n_level.bit_length() - 1) and n_dev <= 64
    low_bits = n_level.bit_length() - 1
    flips = ([(1 - 2 * lax.rem(lv // (1 << i), 2)) * (1 << i) for i in range(low_bits)]
             + [(1 - 2 * lax.rem(sp // (1 << i), 2)) * (1 << i) for i in range(bits - low_bits)]) if mirror else []

    def partner(d):
        if not mirror:
            q = lax.rem(dev + d, n_dev)
            return {"space": q // n_level, "level": lax.rem(q, n_level)}
        if not isinstance(d, int):
            return {"space": 0, "level": 0}
        low = low_bits
        flip = [sum((flips[i] for i in bit if d >> i & 1), 0) for bit in (range(low), range(low, bits))]
        return {"space": sp + flip[1], "level": lv + flip[0]}

    def line_copy(d):
        return pltpu.make_async_remote_copy(
            src_ref=line, dst_ref=lines.at[d - 1], send_sem=line_send, recv_sem=line_recv,
            device_id=partner(d), device_id_type=pl.DeviceIdType.MESH)

    def send_lines():
        if mirror:
            for d in range(n_dev - 1, 0, -1):
                line_copy(d).start()
        else:
            def start(d, _):
                line_copy(d).start()
                return 0

            lax.fori_loop(1, n_dev, start, 0)

    def every_line():
        return pltpu.make_async_remote_copy(
            src_ref=lines, dst_ref=lines, send_sem=line_send, recv_sem=line_recv,
            device_id=partner(1), device_id_type=pl.DeviceIdType.MESH)

    def add_lines():
        if not mirror:
            return lax.fori_loop(0, n_dev - 1, lambda d, total: total + lines[d], line[...])
        terms = [line[...]] + [lines[d] for d in range(n_dev - 1)]
        while len(terms) > 1:
            terms = [sum(terms[i + 1:i + 2], terms[i]) for i in range(0, len(terms), 2)]
        return terms[0]

    def dense(rho, level):
        return level + buoyancy * spread_sum(rho * thickness)

    def stage(s, side, fields, level, heavy):
        for g in range(3):
            own[g, blocks + side] = fields[g]
            out[s, side, g * rows:(g + 1) * rows] = fields[g]
        eta[blocks + side] = level
        out[s, side, 3 * rows:3 * rows + 8] = level
        out_small[s, side, 0] = level[:1]
        out_small[s, side, 1] = heavy[:1]

    def send_out(s):
        for side in range(2):
            @pl.when(has[side])
            def _():
                main_copy(s, side).start()
                for q in others:
                    small_copy(s, side, q, lv).start()

    def close(s):
        for q in others:
            peer_copy(s, q, lv).wait_send()
        for side in range(2):
            @pl.when(has[side])
            def _():
                main_copy(s, side).wait_send()
                for q in others:
                    small_copy(s, side, q, lv).wait_send()

    def gathered(sums, diff, weights):
        east, north, smooth = weights
        return [sums[0] + smooth * diff[0], sums[1] + smooth * diff[1], sums[2] + smooth * diff[2],
                sums[3] + east * diff[2], sums[4] + north * diff[2],
                sums[5] + (east * diff[0] + north * diff[1])]

    def own_parts():
        def body(t, _):
            tiles = [[own[g, b] for b in range(blocks)] for g in range(3)]
            here = [own[g, t] for g in range(3)]
            zero = jnp.zeros((rows, LANES), jnp.float32)
            sums = [zero] * 6
            for k in range(near_count):
                block = block_of[t, k]
                masks = [block == b for b in range(1, blocks)]
                diff = [pick(tiles[g], lanes_of[t, k], masks) - here[g] for g in range(3)]
                sums = gathered(sums, diff, [weight_of[t, k, i] for i in range(3)])
            for i in range(6):
                part[t, i] = sums[i]
            return 0
        several = max(d for d in (1, 2, 5) if targets % d == 0)

        def bodies(i, _):
            for j in range(several):
                body(i * several + j, 0)
            return 0
        lax.fori_loop(0, targets // several, bodies, 0)

    def own_surface(s):
        total = peer_out[s, 0]
        for q in others:
            total = total + peer[s, q]
        q_sum[...] = total
        tiles = [wide(q_sum[t:t + 1, :], 8) for t in range(blocks)]
        for side in range(2):
            lanes, masks = listed(side)
            tiles.append(pick(tiles[:blocks], lanes[:8], [mask[:8] for mask in masks]))
        for t in range(targets):
            q_of[t] = tiles[t]
            block = pack_block[t]
            diff = pick(tiles[:blocks], pack_lanes[t], [block == b for b in range(1, blocks)]) - tiles[t]
            q_part[t, 0] = pack_weight[t, 0] * diff
            q_part[t, 1] = pack_weight[t, 1] * diff

    def receive(s):
        for side in range(2):
            @pl.when(has[side])
            def _():
                main_copy(s, 1 - side).wait_recv()
                for q in others:
                    small_copy(s, 1 - side, q, q).wait_recv()
        for side in range(2):
            total = halo[s, side, 3 * rows:3 * rows + 1]
            for q in others:
                total = total + halo_small[s, side, q]
            q_edge[side] = wide(total, 8)

    def advance(s, t):
        edges = [[halo[s, side, g * rows:(g + 1) * rows] for side in range(2)] for g in range(3)]
        here = [own[g, t] for g in range(3)]
        sums = [part[t, i] for i in range(6)]
        for k in range(near_count):
            lanes = lanes_of[t, k]
            upper = block_of[t, k] == blocks + 1
            diff = [jnp.where(upper, lane_gather(edges[g][1], lanes), lane_gather(edges[g][0], lanes)) - here[g]
                    for g in range(3)]
            sums = gathered(sums, diff, [weight_of[t, k, 3 + i] for i in range(3)])
        lap0, lap1, lap2, east2, north2, flow = sums
        lanes = pack_lanes[t]
        diff = jnp.where(pack_block[t] == blocks + 1, lane_gather(q_edge[1], lanes),
                         lane_gather(q_edge[0], lanes)) - q_of[t]
        slope0 = spread_sum(q_part[t, 0] + pack_weight[t, 3] * diff)
        slope1 = spread_sum(q_part[t, 1] + pack_weight[t, 4] * diff)
        bottom, turn = bot_of[t], cor_of[t]
        drag = jnp.where(level_ids == bottom - 1, drag_rate, 0.0)
        u, v, rho = here
        east3, north3 = thickness * east2, thickness * north2
        east3 = slope0 + buoyancy * (running_sum(east3, rows, row_ids) - 0.5 * east3)
        north3 = slope1 + buoyancy * (running_sum(north3, rows, row_ids) - 0.5 * north3)
        push0 = -east3 + turn * v + lap0 - drag * u
        push1 = -north3 - turn * u + lap1 - drag * v
        wet = level_ids < bottom
        fields = (jnp.where(wet, u + time_step * push0, 0.0), jnp.where(wet, v + time_step * push1, 0.0),
                  rho + time_step * (lap2 - u * east2 - v * north2))
        diverge = spread_sum(thickness * flow)
        level = eta[t] - time_step * jnp.where(bottom[:8] > 0, diverge, 0.0)
        return fields, diverge, level, dense(fields[2], level)

    def transport(fields):
        return jnp.where(odd, spread_sum(thickness * fields[1]), spread_sum(thickness * fields[0]))

    def finish_listed(s):
        for side in range(2):
            fields, _, level, heavy = advance(s, blocks + side)
            stage(s + 1, side, fields, level, heavy)

    def finish(s):
        def body(t, carry):
            volume, light, heavy = carry
            fields, diverge, level, more = advance(s, t)
            for g in range(3):
                own[g, t] = fields[g]
            flow[t] = transport(fields)
            eta[t] = level
            return (volume + wide(area[pl.ds(t, 1), :], 8) * diverge,
                    jnp.where(eight == t, level, light), jnp.where(eight == t, more, heavy))

        zero = jnp.zeros((8, LANES), jnp.float32)
        volume, light, heavy = lax.fori_loop(0, blocks, body, (zero, zero, zero), unroll=True)
        vol[...] = jnp.where(eight == s, volume, vol[...])
        peer_out[s + 1, 0] = light
        peer_out[s + 1, 1] = heavy

    def make_adjoint(s):
        ids = lax.broadcasted_iota(jnp.int32, (2 * LANES, LANES), 0).astype(jnp.bfloat16)

        def body(t, total):
            weight = wide(area[pl.ds(t, 1), :], 8)
            for k in range(near_count):
                slot = jnp.maximum((block_of[t, k][:1] - blocks) * LANES + lanes_of[t, k][:1], -1)
                slot = jnp.broadcast_to(slot.astype(jnp.bfloat16), ids.shape)
                hot = jnp.where(ids == slot, jnp.bfloat16(1), jnp.bfloat16(0))
                value = jnp.where(odd, weight_of[t, k, 4][:8], weight_of[t, k, 3][:8]) * weight
                high = value.astype(jnp.bfloat16).astype(jnp.float32)
                value = value - high
                middle = value.astype(jnp.bfloat16).astype(jnp.float32)
                value = value - middle
                value = jnp.where(eight < 2, high, jnp.where(eight < 4, middle, jnp.where(eight < 6, value, 0.0)))
                total = total + lax.dot_general(
                    value.astype(jnp.bfloat16), hot, (((1,), (1,)), ((), ())), preferred_element_type=jnp.float32)
            return total

        half = -(-blocks // 2)
        total = lax.fori_loop(s * half, jnp.minimum((s + 1) * half, blocks), body, adjoint_sum[...])
        adjoint_sum[...] = total
        total = total + pltpu.roll(total, 4, 0)
        total = total + pltpu.roll(total, 2, 0)
        for side in range(2):
            adjoint[side] = total[:, side * LANES:(side + 1) * LANES]
            @pl.when(jnp.logical_and(has[side], s == 1))
            def _():
                adjoint_copy(side).start()

    def add_early():
        sums = jnp.sum(vol[...], axis=1, keepdims=True)
        total = jnp.zeros((1, LANES), jnp.float32)
        for i in (*range(STEPS - 2), STEPS):
            total = jnp.where(lane_ids == i, sums[i:i + 1], total)
        vol_line[...] = total

    def start_late():
        for side in range(2):
            @pl.when(has[side])
            def _():
                adjoint_copy(1 - side).wait_recv()
        tiles = [flow[t] for t in range(blocks)]
        volume = jnp.zeros((8, LANES), jnp.float32)
        for t in range(blocks):
            total = jnp.zeros((8, LANES), jnp.float32)
            for j in range(flow_own.shape[1]):
                block = flow_block[t, j]
                found = pick(tiles, flow_lanes[t, j], [block == b for b in range(1, blocks)])
                total = total + (flow_own[t, j] * (found - tiles[t]) - flow_halo[t, j] * tiles[t])
            volume = volume + wide(area[t:t + 1, :], 8) * total
        for side in range(2):
            lanes, masks = listed(side)
            found = pick(tiles, lanes[:8], [mask[:8] for mask in masks])
            volume = volume + jnp.where(eight < 2, adjoint_in[side] * found, 0.0)
        volume = jnp.where(eight == 1, vol[...][STEPS - 2:STEPS - 1], spread_sum(volume))
        line[...] = jnp.where(eight == 0, vol_line[...], volume)[:3]
        hear(rounds - 1)
        send_lines()

    def first(t, carry):
        light, heavy = carry
        here = slice(t * LANES, (t + 1) * LANES)
        bottom = wide(bot[t:t + 1, :])
        bot_of[t] = bottom
        wet = level_ids < bottom
        own[0, t] = jnp.where(wet, vel[0, :, here], 0.0)
        own[1, t] = jnp.where(wet, vel[1, :, here], 0.0)
        own[2, t] = den[:, here]
        level = jnp.where(lv == 0, wide(ele[t:t + 1, :], 8), 0.0)
        eta[t] = level
        more = dense(own[2, t], level)
        small[t] = jnp.where(odd, more, level)
        return jnp.where(eight == t, level, light), jnp.where(eight == t, more, heavy)

    zero = jnp.zeros((8, LANES), jnp.float32)
    light, heavy = zero, zero
    for t in range(blocks):
        light, heavy = first(t, (light, heavy))
    peer_out[0, 0] = light
    peer_out[0, 1] = heavy
    for side in range(2):
        lanes, masks = listed(side)
        fields = [pick([own[g, b] for b in range(blocks)], lanes, masks) for g in range(3)]
        found = pick([small[b] for b in range(blocks)], lanes[:8], [m[:8] for m in masks])
        stage(0, side, fields, wide(found[:1], 8), wide(found[1:2], 8))

    pl.semaphore_wait(barrier, len(others) + n_level * (low + high))
    tell(0)
    send_out(0)
    for q in others:
        peer_copy(0, q, lv).start()
    for i in range(len(loads)):
        if i not in early:
            loads[i].wait()
    lax.fori_loop(0, blocks, prepare, 0)
    wet_area = area[...] * jnp.where(bot[...] > 0, 1.0, 0.0)
    area[...] = wet_area
    count = jnp.where(lv == 0, 1.0, 0.0)
    vol[...] = jnp.where(eight == STEPS, wide(jnp.sum(wet_area, axis=0, keepdims=True), 8) * count, 0.0)
    adjoint_sum[...] = jnp.zeros((8, 2 * LANES), jnp.float32)
    listed_tables()

    each = -(-(rounds - 1) // (STEPS - 1))

    def step(s, _):
        own_parts()

        @pl.when(s < 2)
        def _():
            make_adjoint(s)

        for turn in range(STEPS - 1):
            @pl.when(s == turn)
            def _():
                for j in range(turn * each, min((turn + 1) * each, rounds - 1)):
                    hear(j)
                    tell(j + 1)

        @pl.when(s == STEPS - 2)
        def _():
            add_early()

        for q in others:
            peer_copy(s, q, q).wait_recv()
        own_surface(s)
        receive(s)
        close(s)

        @pl.when(s < STEPS - 2)
        def _():
            finish_listed(s)
            send_out(s + 1)

        finish(s)
        for q in others:
            peer_copy(s + 1, q, lv).start()

        @pl.when(s == STEPS - 2)
        def _():
            start_late()
            finish_listed(s)
            send_out(s + 1)

        return 0

    lax.fori_loop(0, STEPS, step, 0)

    for t in range(blocks):
        here = slice(t * LANES, (t + 1) * LANES)
        vel_out[0, :, here] = own[0, t]
        vel_out[1, :, here] = own[1, t]
        den_out[:, here] = own[2, t]

    level = peer_out[STEPS, 0]
    for q in others:
        peer_copy(STEPS, q, q).wait_recv()
        level = level + peer[STEPS, q]
    for q in others:
        peer_copy(STEPS, q, lv).wait_send()
    for side in range(2):
        @pl.when(has[side])
        def _():
            adjoint_copy(side).wait_send()

    every_line().wait_send()
    every_line().wait_recv()
    total = add_lines()
    early = total[:1]
    area_total = early[:, STEPS:STEPS + 1]
    drifts = early / area_total
    shift = jnp.sum(jnp.where(lane_ids < STEPS - 2, drifts, 0.0), axis=1, keepdims=True)
    last = jnp.sum(total[1:], axis=1, keepdims=True) / area_total
    for i in range(2):
        drifts = jnp.where(lane_ids == STEPS - 2 + i, last[i:i + 1], drifts)
        shift = shift + last[i:i + 1]
    ele_out[...] = level + time_step * shift
    drift_out[...] = drifts


def emit(vel, den, ele, drift, vel_out, den_out, ele_out, drift_out):
    vel_out[...] = vel[...]
    den_out[...] = den[...]
    ele_out[...] = ele[...]
    drift_out[...] = drift[:, :STEPS]


def solution(mesh):
    n_space, n_level = mesh.shape["space"], mesh.shape["level"]
    n_dev = n_space * n_level

    def local(velocity, density, elevation, grad_weights, lap_weights, coriolis,
              node_area, thickness, send_list, neighbours, bottom):
        rows, nodes = density.shape
        blocks = nodes // LANES
        near_count = neighbours.shape[0]
        assert near_count < 8 and rows == 8
        packs = -(-near_count // 4)
        f32, i32 = jnp.float32, jnp.int32
        plane = (blocks, LANES)
        vmem = pl.BlockSpec(memory_space=pltpu.VMEM)
        hbm = pl.BlockSpec(memory_space=pltpu.HBM)
        dma = pltpu.SemaphoreType.DMA
        tile = (rows, LANES)
        pack = (8, LANES)
        arrays = [velocity, density, elevation.reshape(plane), grad_weights.transpose(1, 0, 2), lap_weights,
                  coriolis.reshape(plane), node_area.reshape(plane), thickness, send_list,
                  neighbours, bottom.reshape(plane)]
        arrays = [pltpu.with_memory_space_constraint(a, pltpu.HBM) for a in arrays]
        out = pl.pallas_call(
            functools.partial(kernel, n_space, n_level, rows, blocks, near_count),
            out_shape=(
                jax.ShapeDtypeStruct(velocity.shape, f32),
                jax.ShapeDtypeStruct(density.shape, f32),
                jax.ShapeDtypeStruct(plane, f32),
                jax.ShapeDtypeStruct((1, LANES), f32),
            ),
            in_specs=[hbm] * 11,
            out_specs=(vmem, vmem, vmem, vmem),
            scratch_shapes=[
                pltpu.VMEM((3, blocks + 2) + tile, f32),
                pltpu.VMEM((blocks + 2,) + pack, f32),
                pltpu.VMEM((blocks + 2,) + tile, f32),
                pltpu.VMEM((blocks + 2,) + tile, i32),
                pltpu.VMEM((blocks + 2, near_count) + tile, i32),
                pltpu.VMEM((blocks + 2, near_count) + tile, i32),
                pltpu.VMEM((blocks + 2, near_count, 6) + tile, f32),
                pltpu.VMEM((blocks + 2,) + pack, i32),
                pltpu.VMEM((blocks + 2,) + pack, i32),
                pltpu.VMEM((blocks + 2, 6) + pack, f32),
                pltpu.VMEM((blocks, packs) + pack, i32),
                pltpu.VMEM((blocks, packs) + pack, i32),
                pltpu.VMEM((blocks, packs) + pack, f32),
                pltpu.VMEM((blocks, packs) + pack, f32),
                pltpu.VMEM((blocks + 2, 6) + tile, f32),
                pltpu.VMEM((blocks + 2, 2) + pack, f32),
                pltpu.VMEM((blocks + 2,) + pack, f32),
                pltpu.VMEM((2,) + pack, f32),
                pltpu.VMEM(plane, f32),
                pltpu.VMEM((blocks,) + pack, f32),
                pltpu.VMEM((STEPS, 2, 3 * rows + 8, LANES), f32),
                pltpu.VMEM((STEPS, 2, 2, 1, LANES), f32),
                pltpu.VMEM((STEPS, 2, 3 * rows + 8, LANES), f32),
                pltpu.VMEM((STEPS, 2, n_level, 1, LANES), f32),
                pltpu.VMEM((STEPS + 1, 2) + plane, f32),
                pltpu.VMEM((STEPS + 1, n_level) + plane, f32),
                pltpu.VMEM((blocks,) + pack, f32),
                pltpu.VMEM(pack, f32),
                pltpu.VMEM((1, LANES), f32),
                pltpu.VMEM((3, LANES), f32),
                pltpu.VMEM((n_dev - 1, 3, LANES), f32),
                pltpu.VMEM((8, 2 * LANES), f32),
                pltpu.VMEM((2,) + pack, f32),
                pltpu.VMEM((2,) + pack, f32),
                dma((2,)), dma((2, 2)),
                dma((2, n_level)), dma((2, 2, n_level)),
                dma((n_level,)), dma((2, n_level)),
                dma, dma,
                dma((2,)), dma((2,)),
                pltpu.SemaphoreType.REGULAR(((n_space - 1).bit_length(),)),
                dma((11,)),
                pltpu.SMEM(thickness.shape, f32),
            ] + [pltpu.VMEM(a.shape, a.dtype) for a in arrays[:7] + arrays[8:]],
            compiler_params=pltpu.CompilerParams(
                collective_id=0, has_side_effects=True, vmem_limit_bytes=16 * 2 ** 20),
        )(*arrays)
        out = pl.pallas_call(
            emit,
            out_shape=(
                jax.ShapeDtypeStruct(velocity.shape, f32),
                jax.ShapeDtypeStruct(density.shape, f32),
                jax.ShapeDtypeStruct(plane, f32),
                jax.ShapeDtypeStruct((1, STEPS), f32),
            ),
            in_specs=[vmem] * 4,
            out_specs=(vmem,) * 4,
            compiler_params=pltpu.CompilerParams(vmem_limit_bytes=2 ** 20),
        )(*out)
        return out[0], out[1], out[2].reshape(nodes), out[3].reshape(STEPS)

    return jax.shard_map(
        local,
        mesh=mesh,
        in_specs=(
            P(None, "level", "space"),
            P("level", "space"),
            P("space"),
            P(None, None, "space"),
            P(None, "space"),
            P("space"),
            P("space"),
            P("level"),
            P("space", None),
            P(None, "space"),
            P("space"),
        ),
        out_specs=(P(None, "level", "space"), P("level", "space"), P("space"), P()),
        check_vma=False,
    )
```

```python
import functools

import jax
import jax.numpy as jnp
from jax import lax
from jax.experimental import pallas as pl
from jax.experimental.pallas import tpu as pltpu
from jax.sharding import PartitionSpec as P

STEPS = 4
LANES = 128

time_step = 0.1
buoyancy = 0.5
drag_rate = 0.5


def lane_gather(values, lanes):
    return jnp.take_along_axis(values, lanes, axis=1, mode="promise_in_bounds")


def pick(tiles, lanes, masks):
    found = lane_gather(tiles[0], lanes)
    for tile, mask in zip(tiles[1:], masks):
        found = jnp.where(mask, lane_gather(tile, lanes), found)
    return found


def running_sum(values, rows, row_ids):
    shift = 1
    while shift < rows:
        moved = pltpu.roll(values, shift, 0)
        values = values + jnp.where(row_ids >= shift, moved, 0.0)
        shift *= 2
    return values


def spread_sum(values):
    shift = values.shape[0] // 2
    while shift:
        values = values + pltpu.roll(values, shift, 0)
        shift //= 2
    return values


def kernel(
    n_space, n_level, width, rows, blocks, near_count,
    vel, den, ele, grad, lap, cor, area, thick, send, near, bot,
    vel_out, den_out, ele_out, drift_out,
    own, eta, cor_of, bot_of, lanes_of, block_of, weight_of, pack_lanes, pack_block, pack_weight,
    flow_lanes, flow_block, flow_own, flow_halo,
    part, q_part, q_of, q_edge, q_sum, small, out, out_small, halo, halo_small, peer_out, peer,
    flow, vol, line, lines, adjoint_sum, adjoint, adjoint_in,
    main_send, main_recv, hs_send, hs_recv, peer_send, peer_recv, line_send, line_recv, adj_send, adj_recv, ready,
    load_sem, thick_in, *loaded,
):
    sp = lax.axis_index("space")
    lv = lax.axis_index("level")
    n_dev = n_space * n_level
    dev = sp * n_level + lv
    has = (sp > 0, sp < n_space - 1)
    ends = (sp - 1, sp + 1)
    low = jnp.where(has[0], 1, 0)
    high = jnp.where(has[1], 1, 0)
    others = [lax.rem(lv + d, n_level) for d in range(1, n_level)]
    targets = blocks + 2
    far = jnp.where(lax.rem(sp, width) == 0, 0, 1)
    near_side = 1 - far

    barrier = pltpu.get_barrier_semaphore()

    for side in range(2):
        @pl.when(has[side])
        def _():
            for q in [lv] + others:
                pl.semaphore_signal(barrier, inc=1, device_id={"space": ends[side], "level": q})
    for q in others:
        pl.semaphore_signal(barrier, inc=1, device_id={"space": sp, "level": q})

    rounds = (n_space - 1).bit_length()

    def reached(j):
        return [(sp - (1 << j), sp >= 1 << j), (sp + (1 << j), sp + (1 << j) < n_space)]

    def tell(j):
        for q, there in reached(j):
            @pl.when(there)
            def _():
                pl.semaphore_signal(ready.at[j], inc=1, device_id={"space": q, "level": lv})

    def hear(j):
        pl.semaphore_wait(ready.at[j], sum(jnp.where(there, 1, 0) for _, there in reached(j)))

    loads = [
        pltpu.make_async_copy(ref, buffer, load_sem.at[i])
        for i, (ref, buffer) in enumerate(zip(
            (vel, den, ele, grad, lap, cor, area, thick, send, near, bot),
            loaded[:7] + (thick_in,) + loaded[7:]))
    ]
    for load in loads:
        load.start()

    row_ids = lax.broadcasted_iota(jnp.int32, (rows, LANES), 0)
    eight = lax.broadcasted_iota(jnp.int32, (8, LANES), 0)
    odd = jnp.bitwise_and(eight, 1) == 1
    lane_ids = lax.broadcasted_iota(jnp.int32, (1, LANES), 1)
    level_ids = row_ids + lv * rows

    def wide(row, count=rows):
        return jnp.broadcast_to(row, (count, LANES))

    for side in range(2):
        @pl.when(jnp.logical_not(has[side]))
        def _():
            halo[:, side] = jnp.zeros(halo.shape[:1] + halo.shape[2:], jnp.float32)
            halo_small[:, side] = jnp.zeros(halo_small.shape[:1] + halo_small.shape[2:], jnp.float32)
            adjoint_in[side] = jnp.zeros(adjoint_in.shape[1:], jnp.float32)

    early = (0, 1, 2, 7, 8, 10)
    for i in early:
        loads[i].wait()
    vel, den, ele, grad, lap, cor, area, send, near, bot = loaded

    thickness = jnp.zeros((rows, LANES), jnp.float32)
    for r in range(rows):
        thickness = jnp.where(row_ids == r, thick_in[r], thickness)

    def prepare(t, _):
        here = pl.ds(pl.multiple_of(t * LANES, LANES), LANES)
        bottom = bot_of[t]
        turn = wide(cor[pl.ds(t, 1), :])
        cor_of[t] = turn
        lane_pack = jnp.zeros((8, LANES), jnp.int32)
        block_pack = bottom[:8]
        packs = [jnp.zeros((8, LANES), jnp.float32) for _ in range(9)]
        packs[2] = turn[:8]
        flows = [[jnp.zeros((8, LANES), jnp.int32)] * 2 + [jnp.zeros((8, LANES), jnp.float32)] * 2
                 for _ in range(flow_own.shape[1])]
        for k in range(near_count):
            slot = wide(near[k:k + 1, here])
            block = lax.shift_right_logical(slot, 7)
            lanes = jnp.bitwise_and(slot, LANES - 1)
            inside = block < blocks
            below = jnp.where(block == blocks, low, 0) > 0
            above = jnp.where(block == blocks + 1, high, 0) > 0
            lanes_of[t, k] = lanes
            block_of[t, k] = block
            values = (wide(grad[k, 0:1, here]), wide(grad[k, 1:2, here]), wide(lap[k:k + 1, here]))
            picked = [jnp.where(mask, value, 0.0) for mask in (inside, below, above) for value in values]
            for i in range(9):
                weight_of[t, k, i] = picked[i]
            mine = eight == k
            lane_pack = jnp.where(mine, lanes[:8], lane_pack)
            block_pack = jnp.where(mine, block[:8], block_pack)
            packs = [jnp.where(mine, value[:8], pack) for value, pack in zip(picked, packs)]
            flow = flows[k // 4]
            first = 2 * (k % 4)
            pair = jnp.logical_or(eight == first, eight == first + 1)
            flow[0] = jnp.where(pair, lanes[:8], flow[0])
            flow[1] = jnp.where(pair, block[:8], flow[1])
            flow[2] = jnp.where(pair, jnp.where(odd, picked[1][:8], picked[0][:8]), flow[2])
            flow[3] = jnp.where(pair, jnp.where(odd, (picked[4] + picked[7])[:8], (picked[3] + picked[6])[:8]), flow[3])
        pack_lanes[t] = lane_pack
        pack_block[t] = block_pack
        for i in range(9):
            pack_weight[t, i] = packs[i]
        for j in range(flow_own.shape[1]):
            flow_lanes[t, j], flow_block[t, j], flow_own[t, j], flow_halo[t, j] = flows[j]
        return 0


    def listed(side):
        slot = wide(send[:, side * LANES:(side + 1) * LANES])
        block = lax.shift_right_logical(slot, 7)
        return jnp.bitwise_and(slot, LANES - 1), [block == b for b in range(1, blocks)]

    def listed_tables():
        for side in range(2):
            t = blocks + side
            lanes, masks = listed(side)
            lanes, masks = lanes[:8], [mask[:8] for mask in masks]
            found_lanes = pick([pack_lanes[b] for b in range(blocks)], lanes, masks)
            found_block = pick([pack_block[b] for b in range(blocks)], lanes, masks)
            found = [pick([pack_weight[b, i] for b in range(blocks)], lanes, masks) for i in range(9)]
            pack_lanes[t] = found_lanes
            pack_block[t] = found_block
            for i in range(9):
                pack_weight[t, i] = found[i]
            bot_of[t] = wide(found_block[7:8])
            cor_of[t] = wide(found[2][7:8])
            for k in range(near_count):
                lanes_of[t, k] = wide(found_lanes[k:k + 1])
                block_of[t, k] = wide(found_block[k:k + 1])
                for i in range(9):
                    weight_of[t, k, i] = wide(found[i][k:k + 1])

    def version(q):
        return jnp.where(q > lv, 1, 0)

    def main_copy(s, side):
        return pltpu.make_async_remote_copy(
            src_ref=out.at[s, side], dst_ref=halo.at[s, 1 - side],
            send_sem=main_send.at[side], recv_sem=main_recv.at[lax.rem(s, 2), 1 - side],
            device_id={"space": ends[side], "level": lv}, device_id_type=pl.DeviceIdType.MESH)

    def small_copy(s, side, q, slot):
        return pltpu.make_async_remote_copy(
            src_ref=out_small.at[s, side, version(q)], dst_ref=halo_small.at[s, 1 - side, slot],
            send_sem=hs_send.at[side, q], recv_sem=hs_recv.at[lax.rem(s, 2), 1 - side, slot],
            device_id={"space": ends[side], "level": q}, device_id_type=pl.DeviceIdType.MESH)

    def main_wait(s, side):
        return pltpu.make_async_remote_copy(
            src_ref=out.at[s, side], dst_ref=halo.at[s, side],
            send_sem=main_send.at[side], recv_sem=main_recv.at[lax.rem(s, 2), side],
            device_id={"space": sp - 1 + 2 * side, "level": lv}, device_id_type=pl.DeviceIdType.MESH)

    def small_wait(s, side, q):
        return pltpu.make_async_remote_copy(
            src_ref=out_small.at[s, side, 0], dst_ref=halo_small.at[s, side, q],
            send_sem=hs_send.at[side, q], recv_sem=hs_recv.at[lax.rem(s, 2), side, q],
            device_id={"space": sp - 1 + 2 * side, "level": q}, device_id_type=pl.DeviceIdType.MESH)

    def adjoint_copy(side):
        return pltpu.make_async_remote_copy(
            src_ref=adjoint.at[side], dst_ref=adjoint_in.at[1 - side],
            send_sem=adj_send.at[side], recv_sem=adj_recv.at[1 - side],
            device_id={"space": ends[side], "level": lv}, device_id_type=pl.DeviceIdType.MESH)

    def peer_copy(s, q, slot):
        return pltpu.make_async_remote_copy(
            src_ref=peer_out.at[s, jnp.where(s < STEPS, version(q), 0)], dst_ref=peer.at[s, slot],
            send_sem=peer_send.at[q], recv_sem=peer_recv.at[lax.rem(s, 2), slot],
            device_id={"space": sp, "level": q}, device_id_type=pl.DeviceIdType.MESH)

    bits = n_dev.bit_length() - 1
    mirror = n_dev == 1 << bits and n_level == 1 << (n_level.bit_length() - 1) and n_dev <= 64
    low_bits = n_level.bit_length() - 1
    flips = ([(1 - 2 * lax.rem(lv // (1 << i), 2)) * (1 << i) for i in range(low_bits)]
             + [(1 - 2 * lax.rem(sp // (1 << i), 2)) * (1 << i) for i in range(bits - low_bits)]) if mirror else []

    def partner(d):
        if not mirror:
            q = lax.rem(dev + d, n_dev)
            return {"space": q // n_level, "level": lax.rem(q, n_level)}
        if not isinstance(d, int):
            return {"space": 0, "level": 0}
        low = low_bits
        flip = [sum((flips[i] for i in bit if d >> i & 1), 0) for bit in (range(low), range(low, bits))]
        return {"space": sp + flip[1], "level": lv + flip[0]}

    def line_copy(d):
        return pltpu.make_async_remote_copy(
            src_ref=line, dst_ref=lines.at[d - 1], send_sem=line_send, recv_sem=line_recv,
            device_id=partner(d), device_id_type=pl.DeviceIdType.MESH)

    def send_lines():
        if mirror:
            for d in range(n_dev - 1, 0, -1):
                line_copy(d).start()
        else:
            def start(d, _):
                line_copy(d).start()
                return 0

            lax.fori_loop(1, n_dev, start, 0)

    def every_line():
        return pltpu.make_async_remote_copy(
            src_ref=lines, dst_ref=lines, send_sem=line_send, recv_sem=line_recv,
            device_id=partner(1), device_id_type=pl.DeviceIdType.MESH)

    def add_lines():
        if not mirror:
            return lax.fori_loop(0, n_dev - 1, lambda d, total: total + lines[d], line[...])
        terms = [line[...]] + [lines[d] for d in range(n_dev - 1)]
        while len(terms) > 1:
            terms = [sum(terms[i + 1:i + 2], terms[i]) for i in range(0, len(terms), 2)]
        return terms[0]

    def dense(rho, level):
        return level + buoyancy * spread_sum(rho * thickness)

    def stage(s, side, fields, level, heavy):
        for g in range(3):
            own[g, blocks + side] = fields[g]
            out[s, side, g * rows:(g + 1) * rows] = fields[g]
        eta[blocks + side] = level
        out[s, side, 3 * rows:3 * rows + 8] = level
        out_small[s, side, 0] = level[:1]
        out_small[s, side, 1] = heavy[:1]

    def send_out(s):
        for side in range(2):
            @pl.when(has[side])
            def _():
                main_copy(s, side).start()
                for q in others:
                    small_copy(s, side, q, lv).start()

    def close(s):
        for q in others:
            peer_copy(s, q, lv).wait_send()
        for side in range(2):
            @pl.when(has[side])
            def _():
                main_copy(s, side).wait_send()
                for q in others:
                    small_copy(s, side, q, lv).wait_send()

    def gathered(sums, diff, weights):
        east, north, smooth = weights
        return [sums[0] + smooth * diff[0], sums[1] + smooth * diff[1], sums[2] + smooth * diff[2],
                sums[3] + east * diff[2], sums[4] + north * diff[2],
                sums[5] + (east * diff[0] + north * diff[1])]

    def own_parts():
        def body(t, _):
            tiles = [[own[g, b] for b in range(blocks)] for g in range(3)]
            here = [own[g, t] for g in range(3)]
            zero = jnp.zeros((rows, LANES), jnp.float32)
            sums = [zero] * 6
            for k in range(near_count):
                block = block_of[t, k]
                masks = [block == b for b in range(1, blocks)]
                diff = [pick(tiles[g], lanes_of[t, k], masks) - here[g] for g in range(3)]
                sums = gathered(sums, diff, [weight_of[t, k, i] for i in range(3)])
            for i in range(6):
                part[t, i] = sums[i]
            return 0
        several = max(d for d in (1, 2, 5) if targets % d == 0)

        def bodies(i, _):
            for j in range(several):
                body(i * several + j, 0)
            return 0
        lax.fori_loop(0, targets // several, bodies, 0)

    def own_surface(s):
        total = peer_out[s, 0]
        for q in others:
            total = total + peer[s, q]
        q_sum[...] = total
        tiles = [wide(q_sum[t:t + 1, :], 8) for t in range(blocks)]
        for side in range(2):
            lanes, masks = listed(side)
            tiles.append(pick(tiles[:blocks], lanes[:8], [mask[:8] for mask in masks]))
        for t in range(targets):
            q_of[t] = tiles[t]
            block = pack_block[t]
            diff = pick(tiles[:blocks], pack_lanes[t], [block == b for b in range(1, blocks)]) - tiles[t]
            q_part[t, 0] = pack_weight[t, 0] * diff
            q_part[t, 1] = pack_weight[t, 1] * diff

    def receive(s, side):
        @pl.when(jnp.where(side == 0, low, high) > 0)
        def _():
            main_wait(s, side).wait_recv()
            for q in others:
                small_wait(s, side, q).wait_recv()

        total = halo[s, side, 3 * rows:3 * rows + 1]
        for q in others:
            total = total + halo_small[s, side, q]
        return wide(total, 8)

    def edge_sums(s, side, t, sums):
        here = [own[g, t] for g in range(3)]
        edge = [halo[s, side, g * rows:(g + 1) * rows] for g in range(3)]
        for k in range(near_count):
            lanes = lanes_of[t, k]
            diff = [lane_gather(edge[g], lanes) - here[g] for g in range(3)]
            sums = gathered(sums, diff, [weight_of[t, k, 3 + 3 * side + i] for i in range(3)])
        return sums

    def edge_surface(side, edge, t):
        diff = lane_gather(edge, pack_lanes[t]) - q_of[t]
        return [q_part[t, i] + pack_weight[t, 3 + 3 * side + i] * diff for i in range(2)]

    def near_part(s, t):
        sums = edge_sums(s, near_side, t, [part[t, i] for i in range(6)])
        for i in range(6):
            part[t, i] = sums[i]
        slopes = edge_surface(near_side, q_edge[1], t)
        for i in range(2):
            q_part[t, i] = slopes[i]

    def near_listed(s):
        for side in range(2):
            near_part(s, blocks + side)

    def near_own(s):
        several = max(d for d in (1, 2, 4) if blocks % d == 0)

        def bodies(i, _):
            for j in range(several):
                near_part(s, i * several + j)
            return 0
        lax.fori_loop(0, blocks // several, bodies, 0)

    def advance(s, t, both=False):
        here = [own[g, t] for g in range(3)]
        sums = edge_sums(s, far, t, [part[t, i] for i in range(6)])
        slopes = edge_surface(far, q_edge[0], t)
        if both:
            sums = edge_sums(s, near_side, t, sums)
            slopes = [a + b - q_part[t, i] for i, (a, b) in enumerate(zip(slopes, edge_surface(near_side, q_edge[1], t)))]
        lap0, lap1, lap2, east2, north2, flow = sums
        slope0, slope1 = [spread_sum(slope) for slope in slopes]
        bottom, turn = bot_of[t], cor_of[t]
        drag = jnp.where(level_ids == bottom - 1, drag_rate, 0.0)
        u, v, rho = here
        east3, north3 = thickness * east2, thickness * north2
        east3 = slope0 + buoyancy * (running_sum(east3, rows, row_ids) - 0.5 * east3)
        north3 = slope1 + buoyancy * (running_sum(north3, rows, row_ids) - 0.5 * north3)
        push0 = -east3 + turn * v + lap0 - drag * u
        push1 = -north3 - turn * u + lap1 - drag * v
        wet = level_ids < bottom
        fields = (jnp.where(wet, u + time_step * push0, 0.0), jnp.where(wet, v + time_step * push1, 0.0),
                  rho + time_step * (lap2 - u * east2 - v * north2))
        diverge = spread_sum(thickness * flow)
        level = eta[t] - time_step * jnp.where(bottom[:8] > 0, diverge, 0.0)
        return fields, diverge, level, dense(fields[2], level)

    def transport(fields):
        return jnp.where(odd, spread_sum(thickness * fields[1]), spread_sum(thickness * fields[0]))

    def finish_listed(s):
        for side in range(2):
            fields, _, level, heavy = advance(s, blocks + side)
            stage(s + 1, side, fields, level, heavy)

    def finish(s, both=False):
        def body(t, carry):
            volume, light, heavy = carry
            fields, diverge, level, more = advance(s, t, both)
            for g in range(3):
                own[g, t] = fields[g]
            flow[t] = transport(fields)
            eta[t] = level
            return (volume + wide(area[pl.ds(t, 1), :], 8) * diverge,
                    jnp.where(eight == t, level, light), jnp.where(eight == t, more, heavy))

        zero = jnp.zeros((8, LANES), jnp.float32)
        volume, light, heavy = lax.fori_loop(0, blocks, body, (zero, zero, zero), unroll=True)
        vol[...] = jnp.where(eight == s, volume, vol[...])
        peer_out[s + 1, 0] = light
        peer_out[s + 1, 1] = heavy

    def make_adjoint(s):
        ids = lax.broadcasted_iota(jnp.int32, (2 * LANES, LANES), 0).astype(jnp.bfloat16)

        def body(t, total):
            weight = wide(area[pl.ds(t, 1), :], 8)
            for k in range(near_count):
                slot = jnp.maximum((block_of[t, k][:1] - blocks) * LANES + lanes_of[t, k][:1], -1)
                slot = jnp.broadcast_to(slot.astype(jnp.bfloat16), ids.shape)
                hot = jnp.where(ids == slot, jnp.bfloat16(1), jnp.bfloat16(0))
                value = jnp.where(odd, (weight_of[t, k, 4] + weight_of[t, k, 7])[:8],
                                  (weight_of[t, k, 3] + weight_of[t, k, 6])[:8]) * weight
                high = value.astype(jnp.bfloat16).astype(jnp.float32)
                value = value - high
                middle = value.astype(jnp.bfloat16).astype(jnp.float32)
                value = value - middle
                value = jnp.where(eight < 2, high, jnp.where(eight < 4, middle, jnp.where(eight < 6, value, 0.0)))
                total = total + lax.dot_general(
                    value.astype(jnp.bfloat16), hot, (((1,), (1,)), ((), ())), preferred_element_type=jnp.float32)
            return total

        cut = 3 * blocks // 4
        for turn, spread in ((0, range(cut)), (1, range(cut, blocks))):
            @pl.when(s == turn)
            def _():
                total = adjoint_sum[...]
                for t in spread:
                    total = body(t, total)
                adjoint_sum[...] = total

        total = adjoint_sum[...]
        total = total + pltpu.roll(total, 4, 0)
        total = total + pltpu.roll(total, 2, 0)
        for side in range(2):
            adjoint[side] = total[:, side * LANES:(side + 1) * LANES]
            @pl.when(jnp.logical_and(has[side], s == 1))
            def _():
                adjoint_copy(side).start()

    def start_late():
        for side in range(2):
            @pl.when(has[side])
            def _():
                adjoint_copy(1 - side).wait_recv()
        tiles = [flow[t] for t in range(blocks)]
        volume = jnp.zeros((8, LANES), jnp.float32)
        for t in range(blocks):
            total = jnp.zeros((8, LANES), jnp.float32)
            for j in range(flow_own.shape[1]):
                block = flow_block[t, j]
                found = pick(tiles, flow_lanes[t, j], [block == b for b in range(1, blocks)])
                total = total + (flow_own[t, j] * (found - tiles[t]) - flow_halo[t, j] * tiles[t])
            volume = volume + wide(area[t:t + 1, :], 8) * total
        for side in range(2):
            lanes, masks = listed(side)
            found = pick(tiles, lanes[:8], [mask[:8] for mask in masks])
            volume = volume + jnp.where(eight < 2, adjoint_in[side] * found, 0.0)
        sums = jnp.sum(jnp.where(eight == STEPS - 1, spread_sum(volume), vol[...]), axis=1, keepdims=True)
        total = jnp.zeros((1, LANES), jnp.float32)
        for i in range(STEPS + 1):
            total = jnp.where(lane_ids == i, sums[i:i + 1], total)
        line[...] = total
        hear(rounds - 1)
        send_lines()

    def first(t, carry):
        light, heavy = carry
        here = slice(t * LANES, (t + 1) * LANES)
        bottom = wide(bot[t:t + 1, :])
        bot_of[t] = bottom
        wet = level_ids < bottom
        own[0, t] = jnp.where(wet, vel[0, :, here], 0.0)
        own[1, t] = jnp.where(wet, vel[1, :, here], 0.0)
        own[2, t] = den[:, here]
        level = jnp.where(lv == 0, wide(ele[t:t + 1, :], 8), 0.0)
        eta[t] = level
        more = dense(own[2, t], level)
        small[t] = jnp.where(odd, more, level)
        return jnp.where(eight == t, level, light), jnp.where(eight == t, more, heavy)

    zero = jnp.zeros((8, LANES), jnp.float32)
    light, heavy = zero, zero
    for t in range(blocks):
        light, heavy = first(t, (light, heavy))
    peer_out[0, 0] = light
    peer_out[0, 1] = heavy
    for side in range(2):
        lanes, masks = listed(side)
        fields = [pick([own[g, b] for b in range(blocks)], lanes, masks) for g in range(3)]
        found = pick([small[b] for b in range(blocks)], lanes[:8], [m[:8] for m in masks])
        stage(0, side, fields, wide(found[:1], 8), wide(found[1:2], 8))

    for i in range(len(loads)):
        if i not in early:
            loads[i].wait()
    lax.fori_loop(0, blocks, prepare, 0)
    wet_area = area[...] * jnp.where(bot[...] > 0, 1.0, 0.0)
    area[...] = wet_area
    count = jnp.where(lv == 0, 1.0, 0.0)
    vol[...] = jnp.where(eight == STEPS, wide(jnp.sum(wet_area, axis=0, keepdims=True), 8) * count, 0.0)
    adjoint_sum[...] = jnp.zeros((8, 2 * LANES), jnp.float32)
    listed_tables()

    pl.semaphore_wait(barrier, len(others) + n_level * (low + high))
    tell(0)
    send_out(0)
    for q in others:
        peer_copy(0, q, lv).start()
    each = -(-(rounds - 1) // (STEPS - 1))

    def step(s, _):
        own_parts()

        @pl.when(s < 2)
        def _():
            make_adjoint(s)

        for turn in range(STEPS - 1):
            @pl.when(s == turn)
            def _():
                for j in range(turn * each, min((turn + 1) * each, rounds - 1)):
                    hear(j)
                    tell(j + 1)

        for q in others:
            peer_copy(s, q, q).wait_recv()
        own_surface(s)
        q_edge[1] = receive(s, near_side)

        @pl.when(s < STEPS - 1)
        def _():
            near_listed(s)

        @pl.when(s >= STEPS - 2)
        def _():
            near_own(s)

        close(s)
        q_edge[0] = receive(s, far)

        @pl.when(s < STEPS - 2)
        def _():
            finish_listed(s)
            send_out(s + 1)

        @pl.when(s < STEPS - 2)
        def _():
            finish(s, True)

        @pl.when(s >= STEPS - 2)
        def _():
            finish(s)

        for q in others:
            peer_copy(s + 1, q, lv).start()

        @pl.when(s == STEPS - 2)
        def _():
            start_late()
            finish_listed(s)
            send_out(s + 1)

        return 0

    lax.fori_loop(0, STEPS, step, 0)

    for t in range(blocks):
        here = slice(t * LANES, (t + 1) * LANES)
        vel_out[0, :, here] = own[0, t]
        vel_out[1, :, here] = own[1, t]
        den_out[:, here] = own[2, t]

    level = peer_out[STEPS, 0]
    for q in others:
        peer_copy(STEPS, q, q).wait_recv()
        level = level + peer[STEPS, q]
    for q in others:
        peer_copy(STEPS, q, lv).wait_send()
    for side in range(2):
        @pl.when(has[side])
        def _():
            adjoint_copy(side).wait_send()

    every_line().wait_send()
    every_line().wait_recv()
    total = add_lines()
    drifts = total / total[:, STEPS:STEPS + 1]
    shift = jnp.sum(jnp.where(lane_ids < STEPS, drifts, 0.0), axis=1, keepdims=True)
    ele_out[...] = level + time_step * shift
    drift_out[...] = drifts


def emit(vel, den, ele, drift, vel_out, den_out, ele_out, drift_out):
    vel_out[...] = vel[...]
    den_out[...] = den[...]
    ele_out[...] = ele[...]
    drift_out[...] = drift[:, :STEPS]


def solution(mesh):
    n_space, n_level = mesh.shape["space"], mesh.shape["level"]
    n_dev = n_space * n_level
    width = max(w for w in range(1, n_space + 1) if n_space % w == 0 and w * w <= n_space)

    def local(velocity, density, elevation, grad_weights, lap_weights, coriolis,
              node_area, thickness, send_list, neighbours, bottom):
        rows, nodes = density.shape
        blocks = nodes // LANES
        near_count = neighbours.shape[0]
        assert near_count < 8 and rows == 8 and blocks % 2 == 0
        packs = -(-near_count // 4)
        f32, i32 = jnp.float32, jnp.int32
        plane = (blocks, LANES)
        vmem = pl.BlockSpec(memory_space=pltpu.VMEM)
        hbm = pl.BlockSpec(memory_space=pltpu.HBM)
        dma = pltpu.SemaphoreType.DMA
        tile = (rows, LANES)
        pack = (8, LANES)
        arrays = [velocity, density, elevation.reshape(plane), grad_weights.transpose(1, 0, 2), lap_weights,
                  coriolis.reshape(plane), node_area.reshape(plane), thickness, send_list,
                  neighbours, bottom.reshape(plane)]
        arrays = [pltpu.with_memory_space_constraint(a, pltpu.HBM) for a in arrays]
        out = pl.pallas_call(
            functools.partial(kernel, n_space, n_level, width, rows, blocks, near_count),
            out_shape=(
                jax.ShapeDtypeStruct(velocity.shape, f32),
                jax.ShapeDtypeStruct(density.shape, f32),
                jax.ShapeDtypeStruct(plane, f32),
                jax.ShapeDtypeStruct((1, LANES), f32),
            ),
            in_specs=[hbm] * 11,
            out_specs=(vmem, vmem, vmem, vmem),
            scratch_shapes=[
                pltpu.VMEM((3, blocks + 2) + tile, f32),
                pltpu.VMEM((blocks + 2,) + pack, f32),
                pltpu.VMEM((blocks + 2,) + tile, f32),
                pltpu.VMEM((blocks + 2,) + tile, i32),
                pltpu.VMEM((blocks + 2, near_count) + tile, i32),
                pltpu.VMEM((blocks + 2, near_count) + tile, i32),
                pltpu.VMEM((blocks + 2, near_count, 9) + tile, f32),
                pltpu.VMEM((blocks + 2,) + pack, i32),
                pltpu.VMEM((blocks + 2,) + pack, i32),
                pltpu.VMEM((blocks + 2, 9) + pack, f32),
                pltpu.VMEM((blocks, packs) + pack, i32),
                pltpu.VMEM((blocks, packs) + pack, i32),
                pltpu.VMEM((blocks, packs) + pack, f32),
                pltpu.VMEM((blocks, packs) + pack, f32),
                pltpu.VMEM((blocks + 2, 6) + tile, f32),
                pltpu.VMEM((blocks + 2, 2) + pack, f32),
                pltpu.VMEM((blocks + 2,) + pack, f32),
                pltpu.VMEM((2,) + pack, f32),
                pltpu.VMEM(plane, f32),
                pltpu.VMEM((blocks,) + pack, f32),
                pltpu.VMEM((STEPS, 2, 3 * rows + 8, LANES), f32),
                pltpu.VMEM((STEPS, 2, 2, 1, LANES), f32),
                pltpu.VMEM((STEPS, 2, 3 * rows + 8, LANES), f32),
                pltpu.VMEM((STEPS, 2, n_level, 1, LANES), f32),
                pltpu.VMEM((STEPS + 1, 2) + plane, f32),
                pltpu.VMEM((STEPS + 1, n_level) + plane, f32),
                pltpu.VMEM((blocks,) + pack, f32),
                pltpu.VMEM(pack, f32),
                pltpu.VMEM((1, LANES), f32),
                pltpu.VMEM((n_dev - 1, 1, LANES), f32),
                pltpu.VMEM((8, 2 * LANES), f32),
                pltpu.VMEM((2,) + pack, f32),
                pltpu.VMEM((2,) + pack, f32),
                dma((2,)), dma((2, 2)),
                dma((2, n_level)), dma((2, 2, n_level)),
                dma((n_level,)), dma((2, n_level)),
                dma, dma,
                dma((2,)), dma((2,)),
                pltpu.SemaphoreType.REGULAR(((n_space - 1).bit_length(),)),
                dma((11,)),
                pltpu.SMEM(thickness.shape, f32),
            ] + [pltpu.VMEM(a.shape, a.dtype) for a in arrays[:7] + arrays[8:]],
            compiler_params=pltpu.CompilerParams(
                collective_id=0, has_side_effects=True, vmem_limit_bytes=16 * 2 ** 20),
        )(*arrays)
        out = pl.pallas_call(
            emit,
            out_shape=(
                jax.ShapeDtypeStruct(velocity.shape, f32),
                jax.ShapeDtypeStruct(density.shape, f32),
                jax.ShapeDtypeStruct(plane, f32),
                jax.ShapeDtypeStruct((1, STEPS), f32),
            ),
            in_specs=[vmem] * 4,
            out_specs=(vmem,) * 4,
            compiler_params=pltpu.CompilerParams(vmem_limit_bytes=2 ** 20),
        )(*out)
        return out[0], out[1], out[2].reshape(nodes), out[3].reshape(STEPS)

    return jax.shard_map(
        local,
        mesh=mesh,
        in_specs=(
            P(None, "level", "space"),
            P("level", "space"),
            P("space"),
            P(None, None, "space"),
            P(None, "space"),
            P("space"),
            P("space"),
            P("level"),
            P("space", None),
            P(None, "space"),
            P("space"),
        ),
        out_specs=(P(None, "level", "space"), P("level", "space"), P("space"), P()),
        check_vma=False,
    )
```

```python
import functools

import jax
import jax.numpy as jnp
from jax import lax
from jax.experimental import pallas as pl
from jax.experimental.pallas import tpu as pltpu
from jax.sharding import PartitionSpec as P

STEPS = 4
LANES = 128

time_step = 0.1
buoyancy = 0.5
drag_rate = 0.5


def lane_gather(values, lanes):
    return jnp.take_along_axis(values, lanes, axis=1, mode="promise_in_bounds")


def pick(tiles, lanes, masks):
    found = lane_gather(tiles[0], lanes)
    for tile, mask in zip(tiles[1:], masks):
        found = jnp.where(mask, lane_gather(tile, lanes), found)
    return found


def running_sum(values, rows, row_ids):
    shift = 1
    while shift < rows:
        moved = pltpu.roll(values, shift, 0)
        values = values + jnp.where(row_ids >= shift, moved, 0.0)
        shift *= 2
    return values


def spread_sum(values):
    shift = values.shape[0] // 2
    while shift:
        values = values + pltpu.roll(values, shift, 0)
        shift //= 2
    return values


def kernel(
    n_space, n_level, width, rows, blocks, near_count,
    vel, den, ele, grad, lap, cor, area, thick, send, near, bot,
    vel_out, den_out, ele_out, drift_out,
    own, eta, cor_of, bot_of, lanes_of, block_of, weight_of, pack_lanes, pack_block, pack_weight,
    flow_lanes, flow_block, flow_own, flow_halo,
    part, q_part, q_of, q_edge, q_sum, small, out, out_small, halo, halo_small, peer_out, peer,
    flow, vol, line, lines, adjoint_sum, adjoint, adjoint_in,
    main_send, main_recv, hs_send, hs_recv, peer_send, peer_recv, line_send, line_recv, adj_send, adj_recv, ready,
    load_sem, thick_in, *loaded,
):
    sp = lax.axis_index("space")
    lv = lax.axis_index("level")
    n_dev = n_space * n_level
    dev = sp * n_level + lv
    has = (sp > 0, sp < n_space - 1)
    ends = (sp - 1, sp + 1)
    low = jnp.where(has[0], 1, 0)
    high = jnp.where(has[1], 1, 0)
    others = [lax.rem(lv + d, n_level) for d in range(1, n_level)]
    targets = blocks + 2
    far = jnp.where(lax.rem(sp, width) == 0, 0, 1)
    near_side = 1 - far

    barrier = pltpu.get_barrier_semaphore()

    for side in range(2):
        @pl.when(has[side])
        def _():
            for q in [lv] + others:
                pl.semaphore_signal(barrier, inc=1, device_id={"space": ends[side], "level": q})
    for q in others:
        pl.semaphore_signal(barrier, inc=1, device_id={"space": sp, "level": q})

    rounds = (n_space - 1).bit_length()

    def reached(j):
        return [(sp - (1 << j), sp >= 1 << j), (sp + (1 << j), sp + (1 << j) < n_space)]

    def tell(j):
        for q, there in reached(j):
            @pl.when(there)
            def _():
                pl.semaphore_signal(ready.at[j], inc=1, device_id={"space": q, "level": lv})

    def hear(j):
        pl.semaphore_wait(ready.at[j], sum(jnp.where(there, 1, 0) for _, there in reached(j)))

    loads = [
        pltpu.make_async_copy(ref, buffer, load_sem.at[i])
        for i, (ref, buffer) in enumerate(zip(
            (vel, den, ele, grad, lap, cor, area, thick, send, near, bot),
            loaded[:7] + (thick_in,) + loaded[7:]))
    ]
    for load in loads:
        load.start()

    row_ids = lax.broadcasted_iota(jnp.int32, (rows, LANES), 0)
    eight = lax.broadcasted_iota(jnp.int32, (8, LANES), 0)
    odd = jnp.bitwise_and(eight, 1) == 1
    lane_ids = lax.broadcasted_iota(jnp.int32, (1, LANES), 1)
    level_ids = row_ids + lv * rows

    def wide(row, count=rows):
        return jnp.broadcast_to(row, (count, LANES))

    for side in range(2):
        @pl.when(jnp.logical_not(has[side]))
        def _():
            halo[:, side] = jnp.zeros(halo.shape[:1] + halo.shape[2:], jnp.float32)
            halo_small[:, side] = jnp.zeros(halo_small.shape[:1] + halo_small.shape[2:], jnp.float32)
            adjoint_in[side] = jnp.zeros(adjoint_in.shape[1:], jnp.float32)

    early = (0, 1, 2, 7, 8, 10)
    for i in early:
        loads[i].wait()
    vel, den, ele, grad, lap, cor, area, send, near, bot = loaded

    thickness = jnp.zeros((rows, LANES), jnp.float32)
    for r in range(rows):
        thickness = jnp.where(row_ids == r, thick_in[r], thickness)

    def prepare(t, _):
        here = pl.ds(pl.multiple_of(t * LANES, LANES), LANES)
        bottom = bot_of[t]
        turn = wide(cor[pl.ds(t, 1), :])
        cor_of[t] = turn
        lane_pack = jnp.zeros((8, LANES), jnp.int32)
        block_pack = bottom[:8]
        packs = [jnp.zeros((8, LANES), jnp.float32) for _ in range(9)]
        packs[2] = turn[:8]
        flows = [[jnp.zeros((8, LANES), jnp.int32)] * 2 + [jnp.zeros((8, LANES), jnp.float32)] * 2
                 for _ in range(flow_own.shape[1])]
        for k in range(near_count):
            slot = wide(near[k:k + 1, here])
            block = lax.shift_right_logical(slot, 7)
            lanes = jnp.bitwise_and(slot, LANES - 1)
            inside = block < blocks
            below = jnp.where(block == blocks, low, 0) > 0
            above = jnp.where(block == blocks + 1, high, 0) > 0
            lanes_of[t, k] = lanes
            block_of[t, k] = block
            values = (wide(grad[k, 0:1, here]), wide(grad[k, 1:2, here]), wide(lap[k:k + 1, here]))
            picked = [jnp.where(mask, value, 0.0) for mask in (inside, below, above) for value in values]
            for i in range(9):
                weight_of[t, k, i] = picked[i]
            mine = eight == k
            lane_pack = jnp.where(mine, lanes[:8], lane_pack)
            block_pack = jnp.where(mine, block[:8], block_pack)
            packs = [jnp.where(mine, value[:8], pack) for value, pack in zip(picked, packs)]
            flow = flows[k // 4]
            first = 2 * (k % 4)
            pair = jnp.logical_or(eight == first, eight == first + 1)
            flow[0] = jnp.where(pair, lanes[:8], flow[0])
            flow[1] = jnp.where(pair, block[:8], flow[1])
            flow[2] = jnp.where(pair, jnp.where(odd, picked[1][:8], picked[0][:8]), flow[2])
            flow[3] = jnp.where(pair, jnp.where(odd, (picked[4] + picked[7])[:8], (picked[3] + picked[6])[:8]), flow[3])
        pack_lanes[t] = lane_pack
        pack_block[t] = block_pack
        for i in range(9):
            pack_weight[t, i] = packs[i]
        for j in range(flow_own.shape[1]):
            flow_lanes[t, j], flow_block[t, j], flow_own[t, j], flow_halo[t, j] = flows[j]
        return 0


    def listed(side):
        slot = wide(send[:, side * LANES:(side + 1) * LANES])
        block = lax.shift_right_logical(slot, 7)
        return jnp.bitwise_and(slot, LANES - 1), [block == b for b in range(1, blocks)]

    def listed_tables():
        for side in range(2):
            t = blocks + side
            lanes, masks = listed(side)
            lanes, masks = lanes[:8], [mask[:8] for mask in masks]
            found_lanes = pick([pack_lanes[b] for b in range(blocks)], lanes, masks)
            found_block = pick([pack_block[b] for b in range(blocks)], lanes, masks)
            found = [pick([pack_weight[b, i] for b in range(blocks)], lanes, masks) for i in range(9)]
            pack_lanes[t] = found_lanes
            pack_block[t] = found_block
            for i in range(9):
                pack_weight[t, i] = found[i]
            bot_of[t] = wide(found_block[7:8])
            cor_of[t] = wide(found[2][7:8])
            for k in range(near_count):
                lanes_of[t, k] = wide(found_lanes[k:k + 1])
                block_of[t, k] = wide(found_block[k:k + 1])
                for i in range(9):
                    weight_of[t, k, i] = wide(found[i][k:k + 1])

    def version(q):
        return jnp.where(q > lv, 1, 0)

    def main_copy(s, side):
        return pltpu.make_async_remote_copy(
            src_ref=out.at[s, side], dst_ref=halo.at[s, 1 - side],
            send_sem=main_send.at[side], recv_sem=main_recv.at[lax.rem(s, 2), 1 - side],
            device_id={"space": ends[side], "level": lv}, device_id_type=pl.DeviceIdType.MESH)

    def small_copy(s, side, q, slot):
        return pltpu.make_async_remote_copy(
            src_ref=out_small.at[s, side, version(q)], dst_ref=halo_small.at[s, 1 - side, slot],
            send_sem=hs_send.at[side, q], recv_sem=hs_recv.at[lax.rem(s, 2), 1 - side, slot],
            device_id={"space": ends[side], "level": q}, device_id_type=pl.DeviceIdType.MESH)

    def main_wait(s, side):
        return pltpu.make_async_remote_copy(
            src_ref=out.at[s, side], dst_ref=halo.at[s, side],
            send_sem=main_send.at[side], recv_sem=main_recv.at[lax.rem(s, 2), side],
            device_id={"space": sp - 1 + 2 * side, "level": lv}, device_id_type=pl.DeviceIdType.MESH)

    def small_wait(s, side, q):
        return pltpu.make_async_remote_copy(
            src_ref=out_small.at[s, side, 0], dst_ref=halo_small.at[s, side, q],
            send_sem=hs_send.at[side, q], recv_sem=hs_recv.at[lax.rem(s, 2), side, q],
            device_id={"space": sp - 1 + 2 * side, "level": q}, device_id_type=pl.DeviceIdType.MESH)

    def adjoint_copy(side):
        return pltpu.make_async_remote_copy(
            src_ref=adjoint.at[side], dst_ref=adjoint_in.at[1 - side],
            send_sem=adj_send.at[side], recv_sem=adj_recv.at[1 - side],
            device_id={"space": ends[side], "level": lv}, device_id_type=pl.DeviceIdType.MESH)

    def peer_copy(s, q, slot):
        return pltpu.make_async_remote_copy(
            src_ref=peer_out.at[s, jnp.where(s < STEPS, version(q), 0)], dst_ref=peer.at[s, slot],
            send_sem=peer_send.at[q], recv_sem=peer_recv.at[lax.rem(s, 2), slot],
            device_id={"space": sp, "level": q}, device_id_type=pl.DeviceIdType.MESH)

    bits = n_dev.bit_length() - 1
    mirror = n_dev == 1 << bits and n_level == 1 << (n_level.bit_length() - 1) and n_dev <= 64
    low_bits = n_level.bit_length() - 1
    flips = ([(1 - 2 * lax.rem(lv // (1 << i), 2)) * (1 << i) for i in range(low_bits)]
             + [(1 - 2 * lax.rem(sp // (1 << i), 2)) * (1 << i) for i in range(bits - low_bits)]) if mirror else []

    def partner(d):
        if not mirror:
            q = lax.rem(dev + d, n_dev)
            return {"space": q // n_level, "level": lax.rem(q, n_level)}
        if not isinstance(d, int):
            return {"space": 0, "level": 0}
        low = low_bits
        flip = [sum((flips[i] for i in bit if d >> i & 1), 0) for bit in (range(low), range(low, bits))]
        return {"space": sp + flip[1], "level": lv + flip[0]}

    def line_copy(d):
        return pltpu.make_async_remote_copy(
            src_ref=line, dst_ref=lines.at[d - 1], send_sem=line_send, recv_sem=line_recv,
            device_id=partner(d), device_id_type=pl.DeviceIdType.MESH)

    def send_lines():
        if mirror:
            for d in range(n_dev - 1, 0, -1):
                line_copy(d).start()
        else:
            def start(d, _):
                line_copy(d).start()
                return 0

            lax.fori_loop(1, n_dev, start, 0)

    def every_line():
        return pltpu.make_async_remote_copy(
            src_ref=lines, dst_ref=lines, send_sem=line_send, recv_sem=line_recv,
            device_id=partner(1), device_id_type=pl.DeviceIdType.MESH)

    def add_lines():
        if not mirror:
            return lax.fori_loop(0, n_dev - 1, lambda d, total: total + lines[d], line[...])
        terms = [line[...]] + [lines[d] for d in range(n_dev - 1)]
        while len(terms) > 1:
            terms = [sum(terms[i + 1:i + 2], terms[i]) for i in range(0, len(terms), 2)]
        return terms[0]

    def dense(rho, level):
        return level + buoyancy * spread_sum(rho * thickness)

    def stage(s, side, fields, level, heavy):
        for g in range(3):
            own[g, blocks + side] = fields[g]
            out[s, side, g * rows:(g + 1) * rows] = fields[g]
        eta[blocks + side] = level
        out_small[s, side, 0] = level[:1]
        out_small[s, side, 1] = heavy[:1]

    def send_out(s):
        for side in range(2):
            @pl.when(has[side])
            def _():
                main_copy(s, side).start()
                for q in [lv] + others:
                    small_copy(s, side, q, lv).start()

    def close(s):
        for q in others:
            peer_copy(s, q, lv).wait_send()
        for side in range(2):
            @pl.when(has[side])
            def _():
                main_copy(s, side).wait_send()
                for q in [lv] + others:
                    small_copy(s, side, q, lv).wait_send()

    def gathered(sums, diff, weights):
        east, north, smooth = weights
        return [sums[0] + smooth * diff[0], sums[1] + smooth * diff[1], sums[2] + smooth * diff[2],
                sums[3] + east * diff[2], sums[4] + north * diff[2],
                sums[5] + (east * diff[0] + north * diff[1])]

    def own_parts():
        def body(t, _):
            tiles = [[own[g, b] for b in range(blocks)] for g in range(3)]
            here = [own[g, t] for g in range(3)]
            zero = jnp.zeros((rows, LANES), jnp.float32)
            sums = [zero] * 6
            for k in range(near_count):
                block = block_of[t, k]
                masks = [block == b for b in range(1, blocks)]
                diff = [pick(tiles[g], lanes_of[t, k], masks) - here[g] for g in range(3)]
                sums = gathered(sums, diff, [weight_of[t, k, i] for i in range(3)])
            for i in range(6):
                part[t, i] = sums[i]
            return 0
        several = max(d for d in (1, 2, 5) if targets % d == 0)

        def bodies(i, _):
            for j in range(several):
                body(i * several + j, 0)
            return 0
        lax.fori_loop(0, targets // several, bodies, 0)

    def own_surface(s):
        total = peer_out[s, 0]
        for q in others:
            total = total + peer[s, q]
        q_sum[...] = total
        tiles = [wide(q_sum[t:t + 1, :], 8) for t in range(blocks)]
        for side in range(2):
            lanes, masks = listed(side)
            tiles.append(pick(tiles[:blocks], lanes[:8], [mask[:8] for mask in masks]))
        for t in range(targets):
            q_of[t] = tiles[t]
            block = pack_block[t]
            diff = pick(tiles[:blocks], pack_lanes[t], [block == b for b in range(1, blocks)]) - tiles[t]
            q_part[t, 0] = pack_weight[t, 0] * diff
            q_part[t, 1] = pack_weight[t, 1] * diff

    def receive(s, side):
        @pl.when(jnp.where(side == 0, low, high) > 0)
        def _():
            main_wait(s, side).wait_recv()
            for q in [lv] + others:
                small_wait(s, side, q).wait_recv()

        total = halo_small[s, side, lv]
        for q in others:
            total = total + halo_small[s, side, q]
        return wide(total, 8)

    def edge_sums(s, side, t, sums):
        here = [own[g, t] for g in range(3)]
        edge = [halo[s, side, g * rows:(g + 1) * rows] for g in range(3)]
        for k in range(near_count):
            lanes = lanes_of[t, k]
            diff = [lane_gather(edge[g], lanes) - here[g] for g in range(3)]
            sums = gathered(sums, diff, [weight_of[t, k, 3 + 3 * side + i] for i in range(3)])
        return sums

    def edge_surface(side, edge, t):
        diff = lane_gather(edge, pack_lanes[t]) - q_of[t]
        return [q_part[t, i] + pack_weight[t, 3 + 3 * side + i] * diff for i in range(2)]

    def near_part(s, t):
        sums = edge_sums(s, near_side, t, [part[t, i] for i in range(6)])
        for i in range(6):
            part[t, i] = sums[i]
        slopes = edge_surface(near_side, q_edge[1], t)
        for i in range(2):
            q_part[t, i] = slopes[i]

    def near_listed(s):
        for side in range(2):
            near_part(s, blocks + side)

    def near_own(s):
        several = max(d for d in (1, 2, 4) if blocks % d == 0)

        def bodies(i, _):
            for j in range(several):
                near_part(s, i * several + j)
            return 0
        lax.fori_loop(0, blocks // several, bodies, 0)

    def advance(s, t, both=False):
        here = [own[g, t] for g in range(3)]
        sums = edge_sums(s, far, t, [part[t, i] for i in range(6)])
        slopes = edge_surface(far, q_edge[0], t)
        if both:
            sums = edge_sums(s, near_side, t, sums)
            slopes = [a + b - q_part[t, i] for i, (a, b) in enumerate(zip(slopes, edge_surface(near_side, q_edge[1], t)))]
        lap0, lap1, lap2, east2, north2, flow = sums
        slope0, slope1 = [spread_sum(slope) for slope in slopes]
        bottom, turn = bot_of[t], cor_of[t]
        drag = jnp.where(level_ids == bottom - 1, drag_rate, 0.0)
        u, v, rho = here
        east3, north3 = thickness * east2, thickness * north2
        east3 = slope0 + buoyancy * (running_sum(east3, rows, row_ids) - 0.5 * east3)
        north3 = slope1 + buoyancy * (running_sum(north3, rows, row_ids) - 0.5 * north3)
        push0 = -east3 + turn * v + lap0 - drag * u
        push1 = -north3 - turn * u + lap1 - drag * v
        wet = level_ids < bottom
        fields = (jnp.where(wet, u + time_step * push0, 0.0), jnp.where(wet, v + time_step * push1, 0.0),
                  rho + time_step * (lap2 - u * east2 - v * north2))
        diverge = spread_sum(thickness * flow)
        level = eta[t] - time_step * jnp.where(bottom[:8] > 0, diverge, 0.0)
        return fields, diverge, level, dense(fields[2], level)

    def transport(fields):
        return jnp.where(odd, spread_sum(thickness * fields[1]), spread_sum(thickness * fields[0]))

    def finish_listed(s):
        for side in range(2):
            fields, _, level, heavy = advance(s, blocks + side)
            stage(s + 1, side, fields, level, heavy)

    def finish(s, both=False):
        def body(t, carry):
            volume, light, heavy = carry
            fields, diverge, level, more = advance(s, t, both)
            for g in range(3):
                own[g, t] = fields[g]
            flow[t] = transport(fields)
            eta[t] = level
            return (volume + wide(area[pl.ds(t, 1), :], 8) * diverge,
                    jnp.where(eight == t, level, light), jnp.where(eight == t, more, heavy))

        zero = jnp.zeros((8, LANES), jnp.float32)
        volume, light, heavy = lax.fori_loop(0, blocks, body, (zero, zero, zero), unroll=True)
        vol[...] = jnp.where(eight == s, volume, vol[...])
        peer_out[s + 1, 0] = light
        peer_out[s + 1, 1] = heavy

    def make_adjoint(s):
        ids = lax.broadcasted_iota(jnp.int32, (2 * LANES, LANES), 0).astype(jnp.bfloat16)

        def body(t, total):
            weight = wide(area[pl.ds(t, 1), :], 8)
            for k in range(near_count):
                slot = jnp.maximum((block_of[t, k][:1] - blocks) * LANES + lanes_of[t, k][:1], -1)
                slot = jnp.broadcast_to(slot.astype(jnp.bfloat16), ids.shape)
                hot = jnp.where(ids == slot, jnp.bfloat16(1), jnp.bfloat16(0))
                value = jnp.where(odd, (weight_of[t, k, 4] + weight_of[t, k, 7])[:8],
                                  (weight_of[t, k, 3] + weight_of[t, k, 6])[:8]) * weight
                high = value.astype(jnp.bfloat16).astype(jnp.float32)
                value = value - high
                middle = value.astype(jnp.bfloat16).astype(jnp.float32)
                value = value - middle
                value = jnp.where(eight < 2, high, jnp.where(eight < 4, middle, jnp.where(eight < 6, value, 0.0)))
                total = total + lax.dot_general(
                    value.astype(jnp.bfloat16), hot, (((1,), (1,)), ((), ())), preferred_element_type=jnp.float32)
            return total

        cut = 3 * blocks // 4
        for turn, spread in ((0, range(cut)), (1, range(cut, blocks))):
            @pl.when(s == turn)
            def _():
                total = adjoint_sum[...]
                for t in spread:
                    total = body(t, total)
                adjoint_sum[...] = total

        total = adjoint_sum[...]
        total = total + pltpu.roll(total, 4, 0)
        total = total + pltpu.roll(total, 2, 0)
        for side in range(2):
            adjoint[side] = total[:, side * LANES:(side + 1) * LANES]
            @pl.when(jnp.logical_and(has[side], s == 1))
            def _():
                adjoint_copy(side).start()

    def start_late():
        for side in range(2):
            @pl.when(has[side])
            def _():
                adjoint_copy(1 - side).wait_recv()
        tiles = [flow[t] for t in range(blocks)]
        volume = jnp.zeros((8, LANES), jnp.float32)
        for t in range(blocks):
            total = jnp.zeros((8, LANES), jnp.float32)
            for j in range(flow_own.shape[1]):
                block = flow_block[t, j]
                found = pick(tiles, flow_lanes[t, j], [block == b for b in range(1, blocks)])
                total = total + (flow_own[t, j] * (found - tiles[t]) - flow_halo[t, j] * tiles[t])
            volume = volume + wide(area[t:t + 1, :], 8) * total
        for side in range(2):
            lanes, masks = listed(side)
            found = pick(tiles, lanes[:8], [mask[:8] for mask in masks])
            volume = volume + jnp.where(eight < 2, adjoint_in[side] * found, 0.0)
        sums = jnp.sum(jnp.where(eight == STEPS - 1, spread_sum(volume), vol[...]), axis=1, keepdims=True)
        total = jnp.zeros((1, LANES), jnp.float32)
        for i in range(STEPS + 1):
            total = jnp.where(lane_ids == i, sums[i:i + 1], total)
        line[...] = total
        hear(rounds - 1)
        send_lines()

    def first(t, carry):
        light, heavy = carry
        here = slice(t * LANES, (t + 1) * LANES)
        bottom = wide(bot[t:t + 1, :])
        bot_of[t] = bottom
        wet = level_ids < bottom
        own[0, t] = jnp.where(wet, vel[0, :, here], 0.0)
        own[1, t] = jnp.where(wet, vel[1, :, here], 0.0)
        own[2, t] = den[:, here]
        level = jnp.where(lv == 0, wide(ele[t:t + 1, :], 8), 0.0)
        eta[t] = level
        more = dense(own[2, t], level)
        small[t] = jnp.where(odd, more, level)
        return jnp.where(eight == t, level, light), jnp.where(eight == t, more, heavy)

    zero = jnp.zeros((8, LANES), jnp.float32)
    light, heavy = zero, zero
    for t in range(blocks):
        light, heavy = first(t, (light, heavy))
    peer_out[0, 0] = light
    peer_out[0, 1] = heavy
    for side in range(2):
        lanes, masks = listed(side)
        fields = [pick([own[g, b] for b in range(blocks)], lanes, masks) for g in range(3)]
        found = pick([small[b] for b in range(blocks)], lanes[:8], [m[:8] for m in masks])
        stage(0, side, fields, wide(found[:1], 8), wide(found[1:2], 8))

    for i in range(len(loads)):
        if i not in early:
            loads[i].wait()
    lax.fori_loop(0, blocks, prepare, 0)
    wet_area = area[...] * jnp.where(bot[...] > 0, 1.0, 0.0)
    area[...] = wet_area
    count = jnp.where(lv == 0, 1.0, 0.0)
    vol[...] = jnp.where(eight == STEPS, wide(jnp.sum(wet_area, axis=0, keepdims=True), 8) * count, 0.0)
    adjoint_sum[...] = jnp.zeros((8, 2 * LANES), jnp.float32)
    listed_tables()

    pl.semaphore_wait(barrier, len(others) + n_level * (low + high))
    tell(0)
    send_out(0)
    for q in others:
        peer_copy(0, q, lv).start()
    each = -(-(rounds - 1) // (STEPS - 1))

    def step(s, _):
        own_parts()

        @pl.when(s < 2)
        def _():
            make_adjoint(s)

        for turn in range(STEPS - 1):
            @pl.when(s == turn)
            def _():
                for j in range(turn * each, min((turn + 1) * each, rounds - 1)):
                    hear(j)
                    tell(j + 1)

        for q in others:
            peer_copy(s, q, q).wait_recv()
        own_surface(s)
        q_edge[1] = receive(s, near_side)

        @pl.when(s < STEPS - 1)
        def _():
            near_listed(s)

        @pl.when(s >= STEPS - 2)
        def _():
            near_own(s)

        close(s)
        q_edge[0] = receive(s, far)

        @pl.when(s < STEPS - 2)
        def _():
            finish_listed(s)
            send_out(s + 1)

        @pl.when(s < STEPS - 2)
        def _():
            finish(s, True)

        @pl.when(s >= STEPS - 2)
        def _():
            finish(s)

        for q in others:
            peer_copy(s + 1, q, lv).start()

        @pl.when(s == STEPS - 2)
        def _():
            start_late()
            finish_listed(s)
            send_out(s + 1)

        return 0

    lax.fori_loop(0, STEPS, step, 0)

    for t in range(blocks):
        here = slice(t * LANES, (t + 1) * LANES)
        vel_out[0, :, here] = own[0, t]
        vel_out[1, :, here] = own[1, t]
        den_out[:, here] = own[2, t]

    level = peer_out[STEPS, 0]
    for q in others:
        peer_copy(STEPS, q, q).wait_recv()
        level = level + peer[STEPS, q]
    for q in others:
        peer_copy(STEPS, q, lv).wait_send()
    for side in range(2):
        @pl.when(has[side])
        def _():
            adjoint_copy(side).wait_send()

    every_line().wait_send()
    every_line().wait_recv()
    total = add_lines()
    drifts = total / total[:, STEPS:STEPS + 1]
    shift = jnp.sum(jnp.where(lane_ids < STEPS, drifts, 0.0), axis=1, keepdims=True)
    ele_out[...] = level + time_step * shift
    drift_out[...] = drifts


def emit(vel, den, ele, drift, vel_out, den_out, ele_out, drift_out):
    vel_out[...] = vel[...]
    den_out[...] = den[...]
    ele_out[...] = ele[...]
    drift_out[...] = drift[:, :STEPS]


def solution(mesh):
    n_space, n_level = mesh.shape["space"], mesh.shape["level"]
    n_dev = n_space * n_level
    width = max(w for w in range(1, n_space + 1) if n_space % w == 0 and w * w <= n_space)

    def local(velocity, density, elevation, grad_weights, lap_weights, coriolis,
              node_area, thickness, send_list, neighbours, bottom):
        rows, nodes = density.shape
        blocks = nodes // LANES
        near_count = neighbours.shape[0]
        assert near_count < 8 and rows == 8 and blocks % 2 == 0
        packs = -(-near_count // 4)
        f32, i32 = jnp.float32, jnp.int32
        plane = (blocks, LANES)
        vmem = pl.BlockSpec(memory_space=pltpu.VMEM)
        hbm = pl.BlockSpec(memory_space=pltpu.HBM)
        dma = pltpu.SemaphoreType.DMA
        tile = (rows, LANES)
        pack = (8, LANES)
        arrays = [velocity, density, elevation.reshape(plane), grad_weights.transpose(1, 0, 2), lap_weights,
                  coriolis.reshape(plane), node_area.reshape(plane), thickness, send_list,
                  neighbours, bottom.reshape(plane)]
        arrays = [pltpu.with_memory_space_constraint(a, pltpu.HBM) for a in arrays]
        out = pl.pallas_call(
            functools.partial(kernel, n_space, n_level, width, rows, blocks, near_count),
            out_shape=(
                jax.ShapeDtypeStruct(velocity.shape, f32),
                jax.ShapeDtypeStruct(density.shape, f32),
                jax.ShapeDtypeStruct(plane, f32),
                jax.ShapeDtypeStruct((1, LANES), f32),
            ),
            in_specs=[hbm] * 11,
            out_specs=(vmem, vmem, vmem, vmem),
            scratch_shapes=[
                pltpu.VMEM((3, blocks + 2) + tile, f32),
                pltpu.VMEM((blocks + 2,) + pack, f32),
                pltpu.VMEM((blocks + 2,) + tile, f32),
                pltpu.VMEM((blocks + 2,) + tile, i32),
                pltpu.VMEM((blocks + 2, near_count) + tile, i32),
                pltpu.VMEM((blocks + 2, near_count) + tile, i32),
                pltpu.VMEM((blocks + 2, near_count, 9) + tile, f32),
                pltpu.VMEM((blocks + 2,) + pack, i32),
                pltpu.VMEM((blocks + 2,) + pack, i32),
                pltpu.VMEM((blocks + 2, 9) + pack, f32),
                pltpu.VMEM((blocks, packs) + pack, i32),
                pltpu.VMEM((blocks, packs) + pack, i32),
                pltpu.VMEM((blocks, packs) + pack, f32),
                pltpu.VMEM((blocks, packs) + pack, f32),
                pltpu.VMEM((blocks + 2, 6) + tile, f32),
                pltpu.VMEM((blocks + 2, 2) + pack, f32),
                pltpu.VMEM((blocks + 2,) + pack, f32),
                pltpu.VMEM((2,) + pack, f32),
                pltpu.VMEM(plane, f32),
                pltpu.VMEM((blocks,) + pack, f32),
                pltpu.VMEM((STEPS, 2, 3 * rows, LANES), f32),
                pltpu.VMEM((STEPS, 2, 2, 1, LANES), f32),
                pltpu.VMEM((STEPS, 2, 3 * rows, LANES), f32),
                pltpu.VMEM((STEPS, 2, n_level, 1, LANES), f32),
                pltpu.VMEM((STEPS + 1, 2) + plane, f32),
                pltpu.VMEM((STEPS + 1, n_level) + plane, f32),
                pltpu.VMEM((blocks,) + pack, f32),
                pltpu.VMEM(pack, f32),
                pltpu.VMEM((1, LANES), f32),
                pltpu.VMEM((n_dev - 1, 1, LANES), f32),
                pltpu.VMEM((8, 2 * LANES), f32),
                pltpu.VMEM((2,) + pack, f32),
                pltpu.VMEM((2,) + pack, f32),
                dma((2,)), dma((2, 2)),
                dma((2, n_level)), dma((2, 2, n_level)),
                dma((n_level,)), dma((2, n_level)),
                dma, dma,
                dma((2,)), dma((2,)),
                pltpu.SemaphoreType.REGULAR(((n_space - 1).bit_length(),)),
                dma((11,)),
                pltpu.SMEM(thickness.shape, f32),
            ] + [pltpu.VMEM(a.shape, a.dtype) for a in arrays[:7] + arrays[8:]],
            compiler_params=pltpu.CompilerParams(
                collective_id=0, has_side_effects=True, vmem_limit_bytes=16 * 2 ** 20),
        )(*arrays)
        out = pl.pallas_call(
            emit,
            out_shape=(
                jax.ShapeDtypeStruct(velocity.shape, f32),
                jax.ShapeDtypeStruct(density.shape, f32),
                jax.ShapeDtypeStruct(plane, f32),
                jax.ShapeDtypeStruct((1, STEPS), f32),
            ),
            in_specs=[vmem] * 4,
            out_specs=(vmem,) * 4,
            compiler_params=pltpu.CompilerParams(vmem_limit_bytes=2 ** 20),
        )(*out)
        return out[0], out[1], out[2].reshape(nodes), out[3].reshape(STEPS)

    return jax.shard_map(
        local,
        mesh=mesh,
        in_specs=(
            P(None, "level", "space"),
            P("level", "space"),
            P("space"),
            P(None, None, "space"),
            P(None, "space"),
            P("space"),
            P("space"),
            P("level"),
            P("space", None),
            P(None, "space"),
            P("space"),
        ),
        out_specs=(P(None, "level", "space"), P("level", "space"), P("space"), P()),
        check_vma=False,
    )
```
